32 devices in a mesh: space: 8 (over z, y), level: 4 (over x, core).
Axes of the slice: x: 2, y: 2, z: 4, core: 2. Of those that a mesh axis runs over, the one named last changes fastest.
Arguments:
- grid_latent: bfloat16 [4096, 512], P('space'), may hold values from -6 to 6
- mesh_latent: bfloat16 [4, 64, 512], P('level', 'space'), may hold values from -6 to 6
- grid_output_cotangent: bfloat16 [4096, 512], P('space'), may hold values from -6 to 6
- w_send: bfloat16 [512, 512], replicated, may hold values from -0.25 to 0.25
- w_recv: bfloat16 [512, 512], replicated, may hold values from -0.25 to 0.25
- output_weight: bfloat16 [512, 512], replicated, may hold values from -0.25 to 0.25
- hidden_layer_bias: float32 [512], replicated, may hold values from -4 to 4
- output_norm_gain: float32 [512], replicated, may hold values from 0.1 to 1.9
- edge_sender: int32 [4, 16384], P('level', 'space'), may hold values from 0 to 23
- edge_receiver: int32 [4, 16384], P('level', 'space'), may hold values from 0 to 511
- edge_live: int32 [4, 16384], P('level', 'space'), may hold values 0 or 1
Outputs:
- d_grid: float32 [4096, 512], P(('space', 'level'))
- d_mesh: float32 [4, 64, 512], P('level', 'space')
- d_w_send: bfloat16 [512, 512], replicated
- d_w_recv: bfloat16 [512, 512], replicated
- d_w_out: bfloat16 [512, 512], replicated
- d_bias: float32 [512], replicated
- d_gain: float32 [512], replicated
The draws below stay inside these ranges and needn't reach their ends.
All inputs are finite; a program needn't handle non-finite values. No bound on the sum of `edge_live` on one device may be relied on, other than what follows from the above.
Results may differ from the reference program's by a relative error of at most 0.012.
Values may be sent and summed in bfloat16 or wider, within the bound.
No kernel may reach another device: no remote copies, remote signals or barrier semaphores. Data moves between devices by JAX's collectives and lax.ppermute only.
A program may use at most 64 MiB of HBM per device.

```python
import jax
import jax.numpy as jnp
from jax import lax

D = 512
G_DEV = 512
MESH_DEV = 8
LEVELS = 4
EDGE_SLOTS_SHARD = 2048
GRID = 4096
MESH_ROWS = 64
EDGES = 16384
N_SPACE = 8


def plant(result, stream_key, low, high):
    longest = result.shape.index(max(result.shape))
    spots = []
    for shift in (0, 1):
        where = [jax.random.randint(jax.random.fold_in(stream_key, axis), (), 0, length) for axis, length in enumerate(result.shape)]
        where[longest] = (where[longest] + shift) % result.shape[longest]
        spots.append(tuple(where))
    return result.at[spots[0]].set(low).at[spots[1]].set(high)


def block_levels(own_key, extent, pieces, least, top_value):
    def one(dim, blocks):
        heights = jax.random.uniform(jax.random.fold_in(jax.random.fold_in(own_key, 6), dim), (blocks,), jnp.float32, least / len(pieces), top_value / len(pieces))
        return jnp.repeat(jnp.exp(heights), extent[dim] // blocks).reshape((-1,) + (1,) * (len(extent) - dim - 1))

    loudness = one(*pieces[0])
    for cut in pieces[1:]:
        loudness = loudness * one(*cut)
    return loudness


def centred(own_key, extent, spread, bound, pieces=(), kind=jnp.bfloat16):
    result = spread * jax.random.normal(own_key, extent, jnp.float32)
    if pieces:
        result = result * block_levels(own_key, extent, pieces, -0.22, 0.18)
    return jnp.clip(result, -bound, bound).astype(kind)


def setup_inputs(seed: int = 0) -> dict:
    streams_of = jax.random.split(jax.random.key(seed), 12)
    return {
        "grid_latent": centred(streams_of[0], (GRID, D), 1.0, 6.0, ((0, 8),)),
        "mesh_latent": centred(streams_of[1], (LEVELS, MESH_ROWS, D), 1.0, 6.0, ((0, 4), (1, 8))),
        "grid_output_cotangent": centred(streams_of[2], (GRID, D), 1.0, 6.0, ((0, 8),)),
        "w_send": centred(streams_of[3], (D, D), D ** -0.5, 0.25),
        "w_recv": centred(streams_of[4], (D, D), D ** -0.5, 0.25),
        "output_weight": centred(streams_of[5], (D, D), D ** -0.5, 0.25),
        "hidden_layer_bias": centred(streams_of[6], (D,), 0.7, 4.0, (), jnp.float32),
        "output_norm_gain": jnp.clip(1.0 + 0.18 * jax.random.normal(streams_of[7], (D,), jnp.float32), 0.1, 1.9),
        "edge_sender": plant(jax.random.randint(streams_of[8], (LEVELS, EDGES), 0, 3 * MESH_DEV), jax.random.fold_in(streams_of[8], 1), 0, (3 * MESH_DEV) - 1).astype(jnp.int32),
        "edge_receiver": plant(jax.random.randint(streams_of[9], (LEVELS, EDGES), 0, G_DEV), jax.random.fold_in(streams_of[9], 1), 0, G_DEV - 1).astype(jnp.int32),
        "edge_live": plant((jax.random.randint(streams_of[10], (LEVELS, EDGES), 0, 4) < 3).astype(jnp.int32), jax.random.fold_in(streams_of[10], 1), 0, 1),
    }


def edge_reverse_step(sending_rows, receiver_rows, cotangent_lines, slot_active_flags, output_weight, hidden_layer_bias, output_norm_gain):
    preact = sending_rows + receiver_rows + hidden_layer_bias
    hidden = jax.nn.silu(preact).astype(jnp.bfloat16)
    outer = jnp.dot(hidden, output_weight, preferred_element_type=jnp.float32)
    center = outer - lax.optimization_barrier(jnp.mean(outer, axis=-1, keepdims=True))
    inv_scale = lax.rsqrt(lax.optimization_barrier(jnp.mean(center * center, axis=-1, keepdims=True)) + 1e-05)
    normed = center * inv_scale
    incoming_gradient = cotangent_lines.astype(jnp.float32) * slot_active_flags[:, None].astype(jnp.float32)
    scaled = incoming_gradient * output_norm_gain
    d_outer = inv_scale * (scaled - lax.optimization_barrier(jnp.mean(scaled, axis=-1, keepdims=True)) - normed * lax.optimization_barrier(jnp.mean(scaled * normed, axis=-1, keepdims=True)))
    d_outer_b = d_outer.astype(jnp.bfloat16)
    w_out_grad = jnp.dot(hidden.T, d_outer_b, preferred_element_type=jnp.float32)
    d_hidden = jnp.dot(d_outer_b, output_weight.T, preferred_element_type=jnp.float32)
    sigmoid = jax.nn.sigmoid(preact)
    preactivation_gradient = d_hidden * sigmoid * (1.0 + preact * (1.0 - sigmoid))
    return (preactivation_gradient, w_out_grad, lax.optimization_barrier(jnp.sum(preactivation_gradient, axis=0)), lax.optimization_barrier(jnp.sum(incoming_gradient * normed, axis=0)))

def reference(grid_latent, mesh_latent, grid_output_cotangent, w_send, w_recv, output_weight, hidden_layer_bias, output_norm_gain, edge_sender, edge_receiver, edge_live):
    proj_send = jnp.einsum('lmd,de->lme', mesh_latent.astype(jnp.float32), w_send.astype(jnp.float32)).astype(jnp.bfloat16)
    projected_receiver = jnp.dot(grid_latent, w_recv, preferred_element_type=jnp.float32)
    mesh_levels = []
    grid_total = jnp.zeros((GRID, D), jnp.float32)
    wout_acc = jnp.zeros((D, D), jnp.float32)
    bias_acc = jnp.zeros((D,), jnp.float32)
    gain_acc = jnp.zeros((D,), jnp.float32)
    for level in range(LEVELS):
        level_table = proj_send[level]
        senders = edge_sender[level]
        receivers = edge_receiver[level]
        active_slots = edge_live[level]

        def visit(carry, shard):
            mesh_acc, grid_acc, wout_sum, bias_sum, gain_sum = carry
            start_offset = (shard * EDGE_SLOTS_SHARD).astype(jnp.int32)
            sender_local = lax.dynamic_slice_in_dim(senders, start_offset, EDGE_SLOTS_SHARD)
            recv_local = lax.dynamic_slice_in_dim(receivers, start_offset, EDGE_SLOTS_SHARD)
            slot_active_flags = lax.dynamic_slice_in_dim(active_slots, start_offset, EDGE_SLOTS_SHARD)
            target = shard + sender_local // MESH_DEV - 1
            target = jnp.where((target < 0) | (target >= N_SPACE), shard, target).astype(jnp.int32)
            global_row = (target * MESH_DEV + sender_local % MESH_DEV).astype(jnp.int32)
            receiver_index = (recv_local + shard * G_DEV).astype(jnp.int32)
            sending_rows = level_table[global_row].astype(jnp.float32)
            preactivation_gradient, output_weight_piece, bias_piece, gain_piece = edge_reverse_step(sending_rows, projected_receiver[receiver_index], grid_output_cotangent[receiver_index], slot_active_flags, output_weight, hidden_layer_bias, output_norm_gain)
            mesh_acc = mesh_acc.at[global_row].add(preactivation_gradient)
            grid_acc = grid_acc.at[receiver_index].add(preactivation_gradient)
            return ((mesh_acc, grid_acc, wout_sum + output_weight_piece, bias_sum + bias_piece, gain_sum + gain_piece), None)
        start_carry = (jnp.zeros((MESH_ROWS, D), jnp.float32), jnp.zeros((GRID, D), jnp.float32), wout_acc, bias_acc, gain_acc)
        final, _ = lax.scan(visit, start_carry, jnp.arange(N_SPACE, dtype=jnp.int32))
        mesh_level, grid_level, wout_acc, bias_acc, gain_acc = final
        mesh_levels.append(mesh_level)
        grid_total = grid_total + grid_level.astype(jnp.bfloat16).astype(jnp.float32)
    mesh_sum = jnp.stack(mesh_levels, axis=0).astype(jnp.bfloat16)
    grid_sum = grid_total.astype(jnp.bfloat16)
    d_mesh = jnp.einsum('lmd,ed->lme', mesh_sum.astype(jnp.float32), w_send.astype(jnp.float32))
    d_grid = jnp.dot(grid_sum, w_recv.T, preferred_element_type=jnp.float32)
    d_w_send = jnp.einsum('lmd,lme->de', mesh_latent.astype(jnp.float32), mesh_sum.astype(jnp.float32))
    d_w_recv = jnp.dot(grid_latent.T, grid_sum, preferred_element_type=jnp.float32)
    return (d_grid, d_mesh, d_w_send.astype(jnp.bfloat16), d_w_recv.astype(jnp.bfloat16), wout_acc.astype(jnp.bfloat16), bias_acc, gain_acc)
```

```python
import functools

import jax
import jax.numpy as jnp
from jax import lax
from jax.experimental import pallas as pl
from jax.experimental.pallas import tpu as pltpu
from jax.sharding import PartitionSpec as P

F32 = jnp.float32
BF16 = jnp.bfloat16
ALL = ("space", "level")
LANES = 128
BLOCK = 512
SUB = 256
WINDOW_ROWS = 32
VMEM = 60 * 1024 * 1024


def sliced(width, parts):
    return width % (16 * parts) == 0


def chunk_of(width, parts):
    if not sliced(width, parts):
        return jax.ShapeDtypeStruct((width + 8, width), F32)
    rows = width * width // parts // LANES + 2 * width // LANES
    return jax.ShapeDtypeStruct((parts, rows, LANES), BF16)


def cost(flops, nbytes):
    return pl.CostEstimate(flops=flops, bytes_accessed=nbytes, transcendentals=0)


def mix(a, b, left, right):
    return lax.dot_general(a, b, (((left,), (right,)), ((), ())), preferred_element_type=F32)


def full(array):
    return pl.BlockSpec(array.shape, lambda *_: (0,) * array.ndim)


def rows_of(line, count):
    return [line[:, j * LANES : (j + 1) * LANES] for j in range(count)]


def columns_of(lines):
    used = jnp.concatenate([line.astype(F32) for line in lines], axis=0)
    pad = jnp.zeros((LANES - used.shape[0], LANES), F32)
    turned = jnp.concatenate([used, pad], axis=0).T
    return [turned[:, j : j + 1] for j in range(len(lines))]


def one_hot_rows(columns, width):
    lane = lax.broadcasted_iota(jnp.int32, (LANES, width), 1).astype(F32)
    hot = [jnp.where(lane == column, 1.0, 0.0).astype(BF16) for column in columns]
    return jnp.concatenate(hot, axis=0)


def one_hot_cols(lines, height):
    row = lax.broadcasted_iota(jnp.int32, (height, LANES), 0)
    hot = [jnp.where(row == line, 1.0, 0.0).astype(BF16) for line in lines]
    return jnp.concatenate(hot, axis=1)


def table_rows(sender, mesh_rows, band, shards):
    window = lax.div(sender, mesh_rows)
    target = band + window - 1
    window = jnp.where((target >= 0) & (target < shards), window, 1)
    return window * mesh_rows + lax.rem(sender, mesh_rows)


def groups(x):
    return jnp.sum(x.reshape(x.shape[0] // 8, 8, x.shape[1]), axis=0)


def split(x):
    hi = x.astype(BF16)
    return hi, (x - hi.astype(F32)).astype(BF16)


def store_slabs(out_ref, total, vector, parts):
    rows, width = total.shape
    if not sliced(width, parts):
        out_ref[:rows, :] = total
        out_ref[rows:, :] = jnp.broadcast_to(vector, (8, width))
        return
    own = rows // parts
    tiles = width // LANES
    for j in range(tiles):
        piece = total[:, j * LANES : (j + 1) * LANES].astype(BF16)
        out_ref[:, j * own : (j + 1) * own, :] = piece.reshape(parts, own, LANES)
    hi, lo = split(vector)
    extra = [v[:, j * LANES : (j + 1) * LANES] for v in (hi, lo) for j in range(tiles)]
    extra = jnp.concatenate([v.astype(F32) for v in extra], axis=0).astype(BF16)
    out_ref[:, own * tiles :, :] = jnp.broadcast_to(extra[None], (parts,) + extra.shape)


def gather_kernel(recv_ref, live_ref, lat_ref, cot_ref, w_ref, pre_ref, out_cot_ref, table):
    @pl.when(pl.program_id(0) == 0)
    def _():
        table[...] = jnp.dot(lat_ref[...], w_ref[...], preferred_element_type=F32).astype(BF16)

    pieces = BLOCK // LANES
    recv = recv_ref[...]
    kept = jnp.where(live_ref[...] == 1, recv, -1)
    cols = columns_of(rows_of(recv, pieces) + rows_of(kept, pieces))
    height = lat_ref.shape[0]
    pre = jnp.dot(one_hot_rows(cols[:pieces], height), table[...], preferred_element_type=F32)
    pre_ref[...] = pre.astype(BF16)
    cot = jnp.dot(one_hot_rows(cols[pieces:], height), cot_ref[...], preferred_element_type=F32)
    out_cot_ref[...] = cot.astype(BF16)


def gather(recv, live, lat, cot, w):
    slots = recv.shape[1]
    width = lat.shape[1]
    line = pl.BlockSpec((1, BLOCK), lambda i: (0, i))
    edge = pl.BlockSpec((BLOCK, width), lambda i: (i, 0))
    flops = 4 * slots * width * lat.shape[0]
    return pl.pallas_call(
        gather_kernel,
        grid=(slots // BLOCK,),
        in_specs=[line, line, full(lat), full(cot), full(w)],
        out_specs=[edge, edge],
        out_shape=[jax.ShapeDtypeStruct((slots, width), BF16)] * 2,
        scratch_shapes=[pltpu.VMEM(lat.shape, BF16)],
        compiler_params=pltpu.CompilerParams(vmem_limit_bytes=VMEM),
        cost_estimate=cost(flops, 6 * slots * width),
        name="edge_gather",
    )(recv, live, lat, cot, w)


def forward_kernel(
    shards, levels, parts,
    place_ref, send_ref, pre_ref, cot_ref, lat_ref, wsend_ref, wout_ref, bias_ref, gain_ref,
    wpart_ref, dout_ref, slope_ref, table, wsum, gsum,
):
    step = pl.program_id(0)
    band = place_ref[0]
    level = place_ref[1]
    mesh_rows = lat_ref.shape[1]

    @pl.when(step == 0)
    def _():
        near = [jnp.maximum(band - 1, 0), band, jnp.minimum(band + 1, shards - 1)]
        rows = [lat_ref[at * levels + level].astype(F32) for at in near]
        rows.append(jnp.zeros((WINDOW_ROWS - 3 * mesh_rows, lat_ref.shape[2]), F32))
        rows = jnp.concatenate(rows, axis=0).astype(BF16)
        proj = jnp.dot(rows, wsend_ref[...], preferred_element_type=F32).astype(BF16)
        table[...] = jnp.zeros_like(table)
        table[:WINDOW_ROWS, :] = proj
        wsum[...] = jnp.zeros_like(wsum)
        gsum[...] = jnp.zeros_like(gsum)

    width = wout_ref.shape[0]
    pieces = BLOCK // LANES
    near = table_rows(send_ref[...], mesh_rows, band, shards)
    cols = columns_of(rows_of(near, pieces))
    each = SUB // LANES
    for part in range(BLOCK // SUB):
        at = pl.ds(part * SUB, SUB)
        hot = one_hot_rows(cols[part * each : (part + 1) * each], LANES)
        pre = jnp.dot(hot, table[...], preferred_element_type=F32)
        pre = pre + pre_ref[at, :].astype(F32) + bias_ref[...]
        sig = 0.5 * jnp.tanh(0.5 * pre) + 0.5
        hidden = (pre * sig).astype(BF16)
        slope_ref[at, :] = (sig * (1.0 + pre * (1.0 - sig))).astype(BF16)
        outer = jnp.dot(hidden, wout_ref[...], preferred_element_type=F32)
        center = outer - jnp.sum(outer, axis=-1, keepdims=True) * (1.0 / width)
        var = jnp.sum(center * center, axis=-1, keepdims=True) * (1.0 / width)
        inv = lax.rsqrt(var + 1e-05)
        normed = center * inv
        upstream = cot_ref[at, :].astype(F32)
        scaled = upstream * gain_ref[...]
        mean_s = jnp.sum(scaled, axis=-1, keepdims=True) * (1.0 / width)
        mean_sn = jnp.sum(scaled * normed, axis=-1, keepdims=True) * (1.0 / width)
        d_outer = (inv * (scaled - mean_s - normed * mean_sn)).astype(BF16)
        dout_ref[at, :] = d_outer
        gsum[...] += groups(upstream * normed)
        wsum[...] += mix(hidden, d_outer, 0, 0)

    @pl.when(step == pl.num_programs(0) - 1)
    def _():
        store_slabs(wpart_ref, wsum[...], jnp.sum(gsum[...], axis=0, keepdims=True), parts)


def forward(shards, levels, place, send, pre, cot, lat, wsend, wout, bias, gain):
    slots, width = pre.shape
    parts = shards * levels
    line = pl.BlockSpec((1, BLOCK), lambda i: (0, i))
    edge = pl.BlockSpec((BLOCK, width), lambda i: (i, 0))
    chunk = chunk_of(width, parts)
    return pl.pallas_call(
        functools.partial(forward_kernel, shards, levels, parts),
        grid=(slots // BLOCK,),
        in_specs=[
            pl.BlockSpec(memory_space=pltpu.SMEM), line, edge, edge,
            full(lat), full(wsend), full(wout), full(bias), full(gain),
        ],
        out_specs=[full(chunk), edge, edge],
        out_shape=[
            chunk,
            jax.ShapeDtypeStruct((slots, width), BF16),
            jax.ShapeDtypeStruct((slots, width), BF16),
        ],
        scratch_shapes=[
            pltpu.VMEM((LANES, width), BF16),
            pltpu.VMEM((width, width), F32),
            pltpu.VMEM((8, width), F32),
        ],
        compiler_params=pltpu.CompilerParams(vmem_limit_bytes=VMEM),
        cost_estimate=cost(5 * slots * width * width, 8 * slots * width),
        name="edge_forward",
    )(place, send, pre, cot, lat, wsend, wout, bias, gain)


def backward_kernel(
    shards, mesh_rows, parts,
    place_ref, send_ref, recv_ref, dout_ref, slope_ref, wout_ref, lat_ref,
    vpart_ref, grid_ref, near_ref, gacc, tacc, bacc,
):
    step = pl.program_id(0)

    @pl.when(step == 0)
    def _():
        gacc[...] = jnp.zeros_like(gacc)
        tacc[...] = jnp.zeros_like(tacc)
        bacc[...] = jnp.zeros_like(bacc)

    pieces = BLOCK // LANES
    near = table_rows(send_ref[...], mesh_rows, place_ref[0], shards)
    d_hidden = mix(dout_ref[...], wout_ref[...], 1, 1)
    d_pre = d_hidden * slope_ref[...].astype(F32)
    bacc[...] += groups(d_pre)
    d_pre = d_pre.astype(BF16)
    hot = one_hot_cols(rows_of(recv_ref[...], pieces), lat_ref.shape[0])
    gacc[...] += jnp.dot(hot, d_pre, preferred_element_type=F32)
    hot = one_hot_cols(rows_of(near, pieces), WINDOW_ROWS)
    tacc[...] += jnp.dot(hot, d_pre, preferred_element_type=F32)

    @pl.when(step == pl.num_programs(0) - 1)
    def _():
        rows = gacc[...].astype(BF16)
        grid_ref[...] = rows
        near_ref[...] = tacc[...]
        total = mix(lat_ref[...], rows, 0, 0)
        store_slabs(vpart_ref, total, jnp.sum(bacc[...], axis=0, keepdims=True), parts)


def backward(shards, levels, mesh_rows, place, send, recv, dout, slope, wout, lat):
    slots, width = dout.shape
    parts = shards * levels
    line = pl.BlockSpec((1, BLOCK), lambda i: (0, i))
    edge = pl.BlockSpec((BLOCK, width), lambda i: (i, 0))
    chunk = chunk_of(width, parts)
    return pl.pallas_call(
        functools.partial(backward_kernel, shards, mesh_rows, parts),
        grid=(slots // BLOCK,),
        in_specs=[
            pl.BlockSpec(memory_space=pltpu.SMEM), line, line, edge, edge, full(wout), full(lat),
        ],
        out_specs=[
            full(chunk),
            pl.BlockSpec(lat.shape, lambda i: (0, 0)),
            pl.BlockSpec((WINDOW_ROWS, width), lambda i: (0, 0)),
        ],
        out_shape=[
            chunk,
            jax.ShapeDtypeStruct(lat.shape, BF16),
            jax.ShapeDtypeStruct((WINDOW_ROWS, width), F32),
        ],
        scratch_shapes=[
            pltpu.VMEM(lat.shape, F32),
            pltpu.VMEM((WINDOW_ROWS, width), F32),
            pltpu.VMEM((8, width), F32),
        ],
        compiler_params=pltpu.CompilerParams(vmem_limit_bytes=VMEM),
        cost_estimate=cost(5 * slots * width * width, 4 * slots * width),
        name="edge_backward",
    )(place, send, recv, dout, slope, wout, lat)


def reduce_kernel(
    mesh_rows, w_ref, v_ref, near_ref, below_ref, above_ref, wsend_ref,
    pay_ref, dmesh_ref, dbias_ref, dgain_ref,
):
    width = wsend_ref.shape[0]
    tiles = width // LANES
    copies = pay_ref.shape[0]
    slab = w_ref.shape[1] - 2 * tiles
    pieces = []
    for source, vector in ((w_ref, dgain_ref), (v_ref, dbias_ref)):
        total = jnp.sum(source[...].astype(F32), axis=0)
        pieces.append(total[:slab])
        both = total[slab : slab + tiles] + total[slab + tiles :]
        for j in range(tiles):
            vector[:, j * LANES : (j + 1) * LANES] = both[j : j + 1]
    mesh = near_ref[mesh_rows : 2 * mesh_rows, :] + below_ref[...] + above_ref[...]
    pieces += [mesh[:, j * LANES : (j + 1) * LANES] for j in range(tiles)]
    payload = jnp.concatenate(pieces, axis=0).astype(BF16)
    pay_ref[...] = jnp.broadcast_to(payload[None], (copies,) + payload.shape)
    dmesh_ref[...] = mix(mesh.astype(BF16), wsend_ref[...], 1, 1)


def reduce(shards, mesh_rows, w, v, near, below, above, wsend):
    width = wsend.shape[0]
    tiles = width // LANES
    rows = 2 * (w.shape[1] - 2 * tiles) + mesh_rows * tiles
    return pl.pallas_call(
        functools.partial(reduce_kernel, mesh_rows),
        out_shape=[
            jax.ShapeDtypeStruct((shards, rows, LANES), BF16),
            jax.ShapeDtypeStruct((mesh_rows, width), F32),
            jax.ShapeDtypeStruct((1, width), F32),
            jax.ShapeDtypeStruct((1, width), F32),
        ],
        compiler_params=pltpu.CompilerParams(vmem_limit_bytes=VMEM),
        cost_estimate=cost(2 * w.size, 4 * w.size),
        name="reduce_slabs",
    )(w, v, near, below, above, wsend)


def spread_kernel(levels, mesh_rows, place_ref, lat_ref, *refs):
    parts_refs = refs[:levels]
    dsend_ref, drecv_ref, dout_ref, mesh = refs[levels:]
    width = dsend_ref.shape[0]
    tiles = width // LANES
    shards = parts_refs[0].shape[0]
    own = width // (shards * levels)
    slab = own * tiles
    level = place_ref[1]
    for k, ref in enumerate(parts_refs):
        for s in range(shards):
            part = s * levels + (level ^ k)
            for j in range(tiles):
                cols = pl.ds(j * LANES, LANES)
                rows = pl.ds(pl.multiple_of(part * own, own), own)
                dout_ref[rows, cols] = ref[s, j * own : (j + 1) * own, :]
                drecv_ref[rows, cols] = ref[s, slab + j * own : slab + (j + 1) * own, :]
            tail = ref[s, 2 * slab :, :].astype(F32)
            for j in range(tiles):
                rows = pl.ds(pl.multiple_of(part * mesh_rows, mesh_rows), mesh_rows)
                cols = pl.ds(j * LANES, LANES)
                mesh[rows, cols] = tail[j * mesh_rows : (j + 1) * mesh_rows]
    dsend_ref[...] = mix(lat_ref[...], mesh[...].astype(BF16), 0, 0).astype(BF16)


def spread(levels, mesh_rows, place, lat, received):
    width = lat.shape[1]
    out = jax.ShapeDtypeStruct((width, width), BF16)
    return pl.pallas_call(
        functools.partial(spread_kernel, levels, mesh_rows),
        in_specs=[pl.BlockSpec(memory_space=pltpu.SMEM)]
        + [pl.BlockSpec(memory_space=pltpu.VMEM)] * (1 + levels),
        out_shape=[out, out, out],
        scratch_shapes=[pltpu.VMEM(lat.shape, F32)],
        compiler_params=pltpu.CompilerParams(vmem_limit_bytes=VMEM),
        cost_estimate=cost(2 * lat.size * width, 8 * width * width),
        name="spread_weights",
    )(place, lat, *received)


def to_all(x, axes, count):
    copies = jnp.broadcast_to(x[None], (count,) + x.shape)
    return lax.all_to_all(copies, axes, 0, 0, tiled=False)


def swap(x, axis, bit):
    return lax.ppermute(x, axis, [(i, i ^ bit) for i in range(lax.axis_size(axis))])


def shift(x, axis, step):
    count = lax.axis_size(axis)
    return lax.ppermute(
        x, axis, [(i, i + step) for i in range(count) if 0 <= i + step < count]
    )


def body(
    grid_latent, mesh_latent, grid_output_cotangent, w_send, w_recv, output_weight,
    hidden_layer_bias, output_norm_gain, edge_sender, edge_receiver, edge_live,
):
    shards, levels = lax.axis_size("space"), lax.axis_size("level")
    parts = shards * levels
    width = grid_latent.shape[1]
    grid_rows = grid_latent.shape[0]
    mesh_rows = mesh_latent.shape[1]
    place = jnp.stack([lax.axis_index("space"), lax.axis_index("level")]).astype(jnp.int32)

    lat_all = to_all(mesh_latent[0], ALL, parts)
    pre, cot = gather(edge_receiver, edge_live, grid_latent, grid_output_cotangent, w_recv)
    wpart, dout, slope = forward(
        shards, levels, place, edge_sender, pre, cot, lat_all, w_send, output_weight,
        hidden_layer_bias[None], output_norm_gain[None],
    )
    whole_slabs = sliced(width, parts)
    if whole_slabs:
        wrecv = lax.all_to_all(wpart, ALL, 0, 0, tiled=False)
    vpart, grid_local, near = backward(
        shards, levels, mesh_rows, place, edge_sender, edge_receiver, dout, slope,
        output_weight, grid_latent,
    )
    if whole_slabs:
        vrecv = lax.all_to_all(vpart, ALL, 0, 0, tiled=False)
    below = shift(near[2 * mesh_rows : 3 * mesh_rows], "space", 1)
    above = shift(near[:mesh_rows], "space", -1)
    share = grid_rows // levels
    levels_grid = lax.all_to_all(
        grid_local.reshape(levels, share, width), "level", 0, 0, tiled=False
    )
    grid_acc = jnp.sum(levels_grid.astype(F32), axis=0).astype(BF16)
    d_grid = jnp.dot(grid_acc, w_recv.T, preferred_element_type=F32)

    if not whole_slabs:
        mesh = near[mesh_rows : 2 * mesh_rows] + below + above
        mesh = mesh.astype(BF16)
        d_mesh = mix(mesh, w_send, 1, 1)
        totals = lax.psum((mix(mesh_latent[0], mesh, 0, 0), vpart, wpart), ALL)
        d_w = [total[:width].astype(BF16) for total in totals]
        return (d_grid, d_mesh[None], *d_w, totals[1][width], totals[2][width])

    payload, d_mesh, d_bias, d_gain = reduce(
        shards, mesh_rows, wrecv, vrecv, near, below, above, w_send
    )
    own = lax.all_to_all(payload, "space", 0, 0, tiled=False)
    received = {0: own}
    bit = levels // 2
    while bit:
        for k in list(received):
            received[k | bit] = swap(received[k], "level", bit)
        bit //= 2
    d_w_send, d_w_recv, d_w_out = spread(
        levels, mesh_rows, place, lat_all.reshape(parts * mesh_rows, width),
        [received[k] for k in range(levels)],
    )
    return (d_grid, d_mesh[None], d_w_send, d_w_recv, d_w_out, d_bias[0], d_gain[0])


def solution(mesh):
    return jax.shard_map(
        body,
        mesh=mesh,
        in_specs=(
            P("space", None), P("level", "space", None), P("space", None), P(), P(), P(), P(), P(),
            P("level", "space"), P("level", "space"), P("level", "space"),
        ),
        out_specs=(P(("space", "level"), None), P("level", "space", None), P(), P(), P(), P(), P()),
        check_vma=False,
    )
```

```python
import functools

import jax
import jax.numpy as jnp
from jax import lax
from jax.experimental import pallas as pl
from jax.experimental.pallas import tpu as pltpu
from jax.sharding import Mesh, PartitionSpec as P


F32 = jnp.float32
BF16 = jnp.bfloat16
ALL = ("space", "high", "low")
MOST = ("space", "high")
LANES = 128
BLOCK = 512
SUB = 256
WINDOW_ROWS = 32
VMEM = 60 * 1024 * 1024


def sliced(width, parts):
    return width % (16 * parts) == 0


def chunk_of(width, parts):
    if not sliced(width, parts):
        return jax.ShapeDtypeStruct((width + 8, width), F32)
    rows = width * width // parts // LANES + 2 * width // LANES
    return jax.ShapeDtypeStruct((parts, rows, LANES), BF16)


def cost(flops, nbytes):
    return pl.CostEstimate(flops=flops, bytes_accessed=nbytes, transcendentals=0)


def mix(a, b, left, right):
    return lax.dot_general(a, b, (((left,), (right,)), ((), ())), preferred_element_type=F32)


def full(array):
    return pl.BlockSpec(array.shape, lambda *_: (0,) * array.ndim)


def rows_of(line, count):
    return [line[:, j * LANES : (j + 1) * LANES] for j in range(count)]


def columns_of(lines):
    used = jnp.concatenate([line.astype(F32) for line in lines], axis=0)
    pad = jnp.zeros((LANES - used.shape[0], LANES), F32)
    turned = jnp.concatenate([used, pad], axis=0).T
    return [turned[:, j : j + 1] for j in range(len(lines))]


def one_hot_rows(columns, width):
    lane = lax.broadcasted_iota(jnp.int32, (LANES, width), 1).astype(F32)
    hot = [jnp.where(lane == column, 1.0, 0.0).astype(BF16) for column in columns]
    return jnp.concatenate(hot, axis=0)


def one_hot_cols(lines, height):
    row = lax.broadcasted_iota(jnp.int32, (height, LANES), 0)
    hot = [jnp.where(row == line, 1.0, 0.0).astype(BF16) for line in lines]
    return jnp.concatenate(hot, axis=1)


def table_rows(sender, mesh_rows, band, shards):
    window = lax.div(sender, mesh_rows)
    target = band + window - 1
    window = jnp.where((target >= 0) & (target < shards), window, 1)
    return window * mesh_rows + lax.rem(sender, mesh_rows)


def groups(x):
    return jnp.sum(x.reshape(x.shape[0] // 8, 8, x.shape[1]), axis=0)


def split(x):
    hi = x.astype(BF16)
    return hi, (x - hi.astype(F32)).astype(BF16)


def store_slabs(out_ref, total, vector, parts):
    rows, width = total.shape
    if len(out_ref.shape) == 2:
        out_ref[:rows, :] = total
        out_ref[rows:, :] = jnp.broadcast_to(vector, (8, width))
        return
    own = rows // parts
    tiles = width // LANES
    for j in range(tiles):
        piece = total[:, j * LANES : (j + 1) * LANES].astype(BF16)
        out_ref[:, j * own : (j + 1) * own, :] = piece.reshape(parts, own, LANES)
    hi, lo = split(vector)
    extra = [v[:, j * LANES : (j + 1) * LANES] for v in (hi, lo) for j in range(tiles)]
    extra = jnp.concatenate([v.astype(F32) for v in extra], axis=0).astype(BF16)
    out_ref[:, own * tiles :, :] = jnp.broadcast_to(extra[None], (parts,) + extra.shape)


def gather_kernel(recv_ref, live_ref, lat_ref, cot_ref, w_ref, pre_ref, out_cot_ref, table):
    @pl.when(pl.program_id(0) == 0)
    def _():
        table[...] = jnp.dot(lat_ref[...], w_ref[...], preferred_element_type=F32).astype(BF16)

    pieces = BLOCK // LANES
    recv = recv_ref[...]
    kept = jnp.where(live_ref[...] == 1, recv, -1)
    cols = columns_of(rows_of(recv, pieces) + rows_of(kept, pieces))
    height = lat_ref.shape[0]
    pre = jnp.dot(one_hot_rows(cols[:pieces], height), table[...], preferred_element_type=F32)
    pre_ref[...] = pre.astype(BF16)
    cot = jnp.dot(one_hot_rows(cols[pieces:], height), cot_ref[...], preferred_element_type=F32)
    out_cot_ref[...] = cot.astype(BF16)


def gather(recv, live, lat, cot, w):
    slots = recv.shape[1]
    width = lat.shape[1]
    line = pl.BlockSpec((1, BLOCK), lambda i: (0, i))
    edge = pl.BlockSpec((BLOCK, width), lambda i: (i, 0))
    flops = 4 * slots * width * lat.shape[0]
    return pl.pallas_call(
        gather_kernel,
        grid=(slots // BLOCK,),
        in_specs=[line, line, full(lat), full(cot), full(w)],
        out_specs=[edge, edge],
        out_shape=[jax.ShapeDtypeStruct((slots, width), BF16)] * 2,
        scratch_shapes=[pltpu.VMEM(lat.shape, BF16)],
        compiler_params=pltpu.CompilerParams(vmem_limit_bytes=VMEM),
        cost_estimate=cost(flops, 6 * slots * width),
        name="edge_gather",
    )(recv, live, lat, cot, w)


def forward_kernel(
    shards, parts,
    place_ref, send_ref, pre_ref, cot_ref, lat_ref, pair_ref, other_ref, wsend_ref, wout_ref, bias_ref, gain_ref,
    wpart_ref, dout_ref, slope_ref, table, wsum, gsum,
):
    step = pl.program_id(0)
    band = place_ref[0]
    mesh_rows = lat_ref.shape[0]

    @pl.when(step == 0)
    def _():
        even = lax.rem(band, 2) == 0
        pair = pair_ref[...].astype(F32)
        other = other_ref[...].astype(F32)
        rows = [jnp.where(even, other, pair), lat_ref[...].astype(F32), jnp.where(even, pair, other)]
        rows.append(jnp.zeros((WINDOW_ROWS - 3 * mesh_rows, lat_ref.shape[1]), F32))
        rows = jnp.concatenate(rows, axis=0).astype(BF16)
        proj = jnp.dot(rows, wsend_ref[...], preferred_element_type=F32).astype(BF16)
        table[...] = jnp.zeros_like(table)
        table[:WINDOW_ROWS, :] = proj
        wsum[...] = jnp.zeros_like(wsum)
        gsum[...] = jnp.zeros_like(gsum)

    width = wout_ref.shape[0]
    pieces = BLOCK // LANES
    near = table_rows(send_ref[...], mesh_rows, band, shards)
    cols = columns_of(rows_of(near, pieces))
    each = SUB // LANES
    for part in range(BLOCK // SUB):
        at = pl.ds(part * SUB, SUB)
        hot = one_hot_rows(cols[part * each : (part + 1) * each], LANES)
        pre = jnp.dot(hot, table[...], preferred_element_type=F32)
        pre = pre + pre_ref[at, :].astype(F32) + bias_ref[...]
        sig = 0.5 * jnp.tanh(0.5 * pre) + 0.5
        hidden = (pre * sig).astype(BF16)
        slope_ref[at, :] = (sig * (1.0 + pre * (1.0 - sig))).astype(BF16)
        outer = jnp.dot(hidden, wout_ref[...], preferred_element_type=F32)
        center = outer - jnp.sum(outer, axis=-1, keepdims=True) * (1.0 / width)
        var = jnp.sum(center * center, axis=-1, keepdims=True) * (1.0 / width)
        inv = lax.rsqrt(var + 1e-05)
        normed = center * inv
        upstream = cot_ref[at, :].astype(F32)
        scaled = upstream * gain_ref[...]
        mean_s = jnp.sum(scaled, axis=-1, keepdims=True) * (1.0 / width)
        mean_sn = jnp.sum(scaled * normed, axis=-1, keepdims=True) * (1.0 / width)
        d_outer = (inv * (scaled - mean_s - normed * mean_sn)).astype(BF16)
        dout_ref[at, :] = d_outer
        gsum[...] += groups(upstream * normed)
        wsum[...] += mix(hidden, d_outer, 0, 0)

    @pl.when(step == pl.num_programs(0) - 1)
    def _():
        store_slabs(wpart_ref, wsum[...], jnp.sum(gsum[...], axis=0, keepdims=True), parts)


def forward(shards, levels, place, send, pre, cot, lat, pair, other, wsend, wout, bias, gain):
    slots, width = pre.shape
    parts = shards * levels
    line = pl.BlockSpec((1, BLOCK), lambda i: (0, i))
    edge = pl.BlockSpec((BLOCK, width), lambda i: (i, 0))
    chunk = chunk_of(width, parts)
    return pl.pallas_call(
        functools.partial(forward_kernel, shards, parts),
        grid=(slots // BLOCK,),
        in_specs=[
            pl.BlockSpec(memory_space=pltpu.SMEM), line, edge, edge,
            full(lat), full(pair), full(other), full(wsend), full(wout), full(bias), full(gain),
        ],
        out_specs=[full(chunk), edge, edge],
        out_shape=[
            chunk,
            jax.ShapeDtypeStruct((slots, width), BF16),
            jax.ShapeDtypeStruct((slots, width), BF16),
        ],
        scratch_shapes=[
            pltpu.VMEM((LANES, width), BF16),
            pltpu.VMEM((width, width), F32),
            pltpu.VMEM((8, width), F32),
        ],
        compiler_params=pltpu.CompilerParams(vmem_limit_bytes=VMEM),
        cost_estimate=cost(5 * slots * width * width, 8 * slots * width),
        name="edge_forward",
    )(place, send, pre, cot, lat, pair, other, wsend, wout, bias, gain)


def backward_kernel(
    shards, mesh_rows, sliced_rows,
    place_ref, send_ref, recv_ref, dout_ref, slope_ref, wout_ref, lat_ref,
    vsend_ref, vkeep_ref, gsend_ref, gkeep_ref, own_ref, pair_ref, other_ref,
    gacc, tacc, bacc, total,
):
    step = pl.program_id(0)

    @pl.when(step == 0)
    def _():
        gacc[...] = jnp.zeros_like(gacc)
        tacc[...] = jnp.zeros_like(tacc)
        bacc[...] = jnp.zeros_like(bacc)

    pieces = BLOCK // LANES
    near = table_rows(send_ref[...], mesh_rows, place_ref[0], shards)
    d_hidden = mix(dout_ref[...], wout_ref[...], 1, 1)
    d_pre = d_hidden * slope_ref[...].astype(F32)
    bacc[...] += groups(d_pre)
    d_pre = d_pre.astype(BF16)
    hot = one_hot_cols(rows_of(recv_ref[...], pieces), lat_ref.shape[0])
    gacc[...] += jnp.dot(hot, d_pre, preferred_element_type=F32)
    hot = one_hot_cols(rows_of(near, pieces), WINDOW_ROWS)
    tacc[...] += jnp.dot(hot, d_pre, preferred_element_type=F32)

    @pl.when(step == pl.num_programs(0) - 1)
    def _():
        high, low = place_ref[1], place_ref[2]
        even = lax.rem(place_ref[0], 2) == 0
        below = tacc[:mesh_rows, :]
        above = tacc[2 * mesh_rows : 3 * mesh_rows, :]
        own_ref[...] = tacc[mesh_rows : 2 * mesh_rows, :]
        pair_ref[...] = jnp.where(even, above, below)
        other_ref[...] = jnp.where(even, below, above)
        total[...] = mix(lat_ref[...], gacc[...].astype(BF16), 0, 0)
        bias = jnp.sum(bacc[...], axis=0, keepdims=True)
        half = vkeep_ref.shape[0] - 8
        if sliced_rows:
            mine = pl.multiple_of(low * half, half)
            theirs = pl.multiple_of((1 - low) * half, half)
            vkeep_ref[:half, :] = total[pl.ds(mine, half), :]
            vsend_ref[:half, :] = total[pl.ds(theirs, half), :].astype(BF16)
            hi, lo = split(bias)
            rest = jnp.zeros((6, bias.shape[1]), F32)
            vsend_ref[half:, :] = jnp.concatenate(
                [hi.astype(F32), lo.astype(F32), rest], axis=0
            ).astype(BF16)
        else:
            vkeep_ref[:half, :] = total[...]
            vsend_ref[...] = jnp.zeros_like(vsend_ref)
        vkeep_ref[half:, :] = jnp.broadcast_to(bias, (8, bias.shape[1]))
        share = gkeep_ref.shape[1]
        for k in range(gkeep_ref.shape[0]):
            base = (high ^ k) * 2
            mine = pl.multiple_of((base + low) * share, share)
            theirs = pl.multiple_of((base + 1 - low) * share, share)
            gkeep_ref[k] = gacc[pl.ds(mine, share), :]
            gsend_ref[k] = gacc[pl.ds(theirs, share), :].astype(BF16)


def backward(shards, levels, mesh_rows, place, send, recv, dout, slope, wout, lat):
    slots, width = dout.shape
    sliced_rows = sliced(width, shards * levels)
    line = pl.BlockSpec((1, BLOCK), lambda i: (0, i))
    edge = pl.BlockSpec((BLOCK, width), lambda i: (i, 0))
    half = width // 2 if sliced_rows else width
    grid = (levels // 2, lat.shape[0] // levels, width)
    near = jax.ShapeDtypeStruct((mesh_rows, width), F32)
    outs = [
        jax.ShapeDtypeStruct((width // 2 + 8, width), BF16),
        jax.ShapeDtypeStruct((half + 8, width), F32),
        jax.ShapeDtypeStruct(grid, BF16),
        jax.ShapeDtypeStruct(grid, F32),
        near, near, near,
    ]
    return pl.pallas_call(
        functools.partial(backward_kernel, shards, mesh_rows, sliced_rows),
        grid=(slots // BLOCK,),
        in_specs=[
            pl.BlockSpec(memory_space=pltpu.SMEM), line, line, edge, edge, full(wout), full(lat),
        ],
        out_specs=[full(out) for out in outs],
        out_shape=outs,
        scratch_shapes=[
            pltpu.VMEM(lat.shape, F32),
            pltpu.VMEM((WINDOW_ROWS, width), F32),
            pltpu.VMEM((8, width), F32),
            pltpu.VMEM((width, width), F32),
        ],
        compiler_params=pltpu.CompilerParams(vmem_limit_bytes=VMEM),
        cost_estimate=cost(5 * slots * width * width, 4 * slots * width),
        name="edge_backward",
    )(place, send, recv, dout, slope, wout, lat)


def combine_kernel(parts, vkeep_ref, vrecv_ref, gkeep_ref, grecv_ref, vpart_ref, gsend_ref, gown_ref):
    half = vkeep_ref.shape[0] - 8
    near = vrecv_ref[...].astype(F32)
    bias = vkeep_ref[half : half + 1, :] + near[half : half + 1] + near[half + 1 : half + 2]
    store_slabs(vpart_ref, vkeep_ref[:half, :] + near[:half], bias, parts)
    gown_ref[...] = gkeep_ref[0] + grecv_ref[0].astype(F32)
    gsend_ref[...] = (gkeep_ref[1] + grecv_ref[1].astype(F32)).astype(BF16)


def combine(parts, vkeep, vrecv, gkeep, grecv):
    width = vkeep.shape[1]
    chunk = chunk_of(width, 2 * parts)
    chunk = jax.ShapeDtypeStruct((parts,) + chunk.shape[1:], chunk.dtype)
    return pl.pallas_call(
        functools.partial(combine_kernel, parts),
        out_shape=[
            chunk,
            jax.ShapeDtypeStruct(gkeep.shape[1:], BF16),
            jax.ShapeDtypeStruct(gkeep.shape[1:], F32),
        ],
        compiler_params=pltpu.CompilerParams(vmem_limit_bytes=VMEM),
        cost_estimate=cost(2 * vkeep.size, 8 * vkeep.size),
        name="combine_halves",
    )(vkeep, vrecv, gkeep, grecv)


def sum_slabs(source_ref, vector_ref):
    tiles = vector_ref.shape[1] // LANES
    slab = source_ref.shape[1] - 2 * tiles
    total = jnp.sum(source_ref[...].astype(F32), axis=0)
    both = total[slab : slab + tiles] + total[slab + tiles :]
    for j in range(tiles):
        vector_ref[:, j * LANES : (j + 1) * LANES] = both[j : j + 1]
    return total[:slab]


def first_kernel(w_ref, slab_ref, dgain_ref):
    slab_ref[...] = sum_slabs(w_ref, dgain_ref)


def first_reduce(w, width):
    slab = w.shape[1] - 2 * width // LANES
    return pl.pallas_call(
        first_kernel,
        out_shape=[
            jax.ShapeDtypeStruct((slab, LANES), F32),
            jax.ShapeDtypeStruct((1, width), F32),
        ],
        compiler_params=pltpu.CompilerParams(vmem_limit_bytes=VMEM),
        cost_estimate=cost(2 * w.size, 2 * w.size),
        name="first_slabs",
    )(w)


def tiles_of(rows):
    return [rows[:, j : j + LANES] for j in range(0, rows.shape[1], LANES)]


def second_kernel(
    v_ref, first_ref, lat_ref, own_ref, pair_ref, other_ref, wsend_ref,
    pay_ref, dmesh_ref, dbias_ref,
):
    mesh = own_ref[...] + pair_ref[...] + other_ref[...]
    pieces = [first_ref[...], sum_slabs(v_ref, dbias_ref)]
    pieces += tiles_of(mesh) + tiles_of(lat_ref[...].astype(F32))
    payload = jnp.concatenate(pieces, axis=0).astype(BF16)
    pay_ref[...] = jnp.broadcast_to(payload[None], pay_ref.shape)
    dmesh_ref[...] = mix(mesh.astype(BF16), wsend_ref[...], 1, 1)


def second_reduce(shards, v, first, lat, own, pair, other, wsend):
    mesh_rows, width = lat.shape
    rows = 2 * first.shape[0] + 2 * mesh_rows * width // LANES
    return pl.pallas_call(
        second_kernel,
        out_shape=[
            jax.ShapeDtypeStruct((shards, rows, LANES), BF16),
            jax.ShapeDtypeStruct((mesh_rows, width), F32),
            jax.ShapeDtypeStruct((1, width), F32),
        ],
        compiler_params=pltpu.CompilerParams(vmem_limit_bytes=VMEM),
        cost_estimate=cost(2 * v.size, 4 * v.size),
        name="second_slabs",
    )(v, first, lat, own, pair, other, wsend)


def spread_kernel(levels, mesh_rows, place_ref, *refs):
    parts_refs = refs[:levels]
    dsend_ref, drecv_ref, dout_ref, mesh, lat = refs[levels:]
    width = dsend_ref.shape[0]
    tiles = width // LANES
    shards = parts_refs[0].shape[0]
    own = width // (shards * levels)
    slab = own * tiles
    level = place_ref[1] * 2 + place_ref[2]
    for k, ref in enumerate(parts_refs):
        for s in range(shards):
            at = level ^ k
            part = s * levels + at
            high, low = lax.shift_right_logical(at, 1), at & 1
            place = (low * shards + s) * (levels // 2) + high
            tail = ref[s, 2 * slab :, :].astype(F32)
            rows = pl.ds(pl.multiple_of(part * own, own), own)
            recv_rows = pl.ds(pl.multiple_of(place * own, own), own)
            near = pl.ds(pl.multiple_of(part * mesh_rows, mesh_rows), mesh_rows)
            for j in range(tiles):
                cols = pl.ds(j * LANES, LANES)
                dout_ref[rows, cols] = ref[s, j * own : (j + 1) * own, :]
                drecv_ref[recv_rows, cols] = ref[s, slab + j * own : slab + (j + 1) * own, :]
                mesh[near, cols] = tail[j * mesh_rows : (j + 1) * mesh_rows]
                lat[near, cols] = tail[(tiles + j) * mesh_rows : (tiles + j + 1) * mesh_rows]
    dsend_ref[...] = mix(lat[...].astype(BF16), mesh[...].astype(BF16), 0, 0).astype(BF16)


def spread(width, mesh_rows, place, received):
    levels = len(received)
    rows = received[0].shape[0] * levels * mesh_rows
    out = jax.ShapeDtypeStruct((width, width), BF16)
    return pl.pallas_call(
        functools.partial(spread_kernel, levels, mesh_rows),
        in_specs=[pl.BlockSpec(memory_space=pltpu.SMEM)]
        + [pl.BlockSpec(memory_space=pltpu.VMEM)] * levels,
        out_shape=[out, out, out],
        scratch_shapes=[pltpu.VMEM((rows, width), F32)] * 2,
        compiler_params=pltpu.CompilerParams(vmem_limit_bytes=VMEM),
        cost_estimate=cost(2 * rows * width * width, 8 * width * width),
        name="spread_weights",
    )(place, *received)


def swap(x, axis, bit):
    return lax.ppermute(x, axis, [(i, i ^ bit) for i in range(lax.axis_size(axis))])


def swap_between(x, axis):
    count = lax.axis_size(axis)
    pairs = [(i, i + 1) for i in range(1, count - 1, 2)]
    return lax.ppermute(x, axis, pairs + [(j, i) for i, j in pairs])


def body(
    grid_latent, mesh_latent, grid_output_cotangent, w_send, w_recv, output_weight,
    hidden_layer_bias, output_norm_gain, edge_sender, edge_receiver, edge_live,
):
    shards, levels = lax.axis_size("space"), lax.axis_size("high") * 2
    parts = shards * levels
    width = grid_latent.shape[1]
    mesh_rows = mesh_latent.shape[1]
    lat = mesh_latent[0]
    whole_slabs = sliced(width, parts)
    place = jnp.stack([lax.axis_index(axis) for axis in ALL]).astype(jnp.int32)

    lat_pair = swap(lat, "space", 1)
    lat_other = swap_between(lat, "space")
    pre, cot = gather(edge_receiver, edge_live, grid_latent, grid_output_cotangent, w_recv)
    wpart, dout, slope = forward(
        shards, levels, place, edge_sender, pre, cot, lat, lat_pair, lat_other, w_send,
        output_weight, hidden_layer_bias[None], output_norm_gain[None],
    )
    if whole_slabs:
        wrecv = lax.all_to_all(wpart, ALL, 0, 0, tiled=False)
    vsend, vkeep, gsend, gkeep, own, pair, other = backward(
        shards, levels, mesh_rows, place, edge_sender, edge_receiver, dout, slope,
        output_weight, grid_latent,
    )
    pair = swap(pair, "space", 1)
    other = swap_between(other, "space")

    if not whole_slabs:
        rows = jnp.stack([gkeep.astype(BF16), gsend])
        for k in range(1, levels):
            side = rows[k % 2, k // 2]
            for bit in (1, 2):
                if k & bit:
                    side = swap(side, ("low", "high")[bit // 2], 1)
            gkeep = gkeep.at[0].add(side.astype(F32))
        d_grid = mix(gkeep[0].astype(BF16), w_recv, 1, 1)
        mesh = (own + pair + other).astype(BF16)
        d_mesh = mix(mesh, w_send, 1, 1)
        totals = lax.psum((mix(lat, mesh, 0, 0), vkeep, wpart), ALL)
        d_w = [total[:width].astype(BF16) for total in totals]
        return (d_grid, d_mesh[None], *d_w, totals[1][width], totals[2][width])

    vnear = swap(vsend, "low", 1)
    gnear = swap(gsend, "low", 1)
    vpart, gsend, gown = combine(parts // 2, vkeep, vnear, gkeep, gnear)
    gfar = swap(gsend, "high", 1)
    vrecv = lax.all_to_all(vpart, MOST, 0, 0, tiled=False)
    d_grid = mix((gown + gfar.astype(F32)).astype(BF16), w_recv, 1, 1)
    first, d_gain = first_reduce(wrecv, width)
    payload, d_mesh, d_bias = second_reduce(
        shards, vrecv, first, lat, own, pair, other, w_send
    )
    received = {0: lax.all_to_all(payload, "space", 0, 0, tiled=False)}
    received[2] = swap(received[0], "high", 1)
    received[1] = swap(received[0], "low", 1)
    received[3] = swap(received[2], "low", 1)
    d_w_send, d_w_recv, d_w_out = spread(
        width, mesh_rows, place, [received[k] for k in range(levels)]
    )
    return (d_grid, d_mesh[None], d_w_send, d_w_recv, d_w_out, d_bias[0], d_gain[0])


def solution(mesh):
    shards, levels = mesh.devices.shape
    split_mesh = Mesh(mesh.devices.reshape(shards, levels // 2, 2), ALL)
    level = MOST[1:] + ALL[2:]

    return jax.shard_map(
        body,
        mesh=split_mesh,
        in_specs=(
            P("space", None), P(level, "space", None), P("space", None), P(), P(), P(), P(), P(),
            P(level, "space"), P(level, "space"), P(level, "space"),
        ),
        out_specs=(P(ALL, None), P(level, "space", None), P(), P(), P(), P(), P()),
        check_vma=False,
    )
```

```python
import functools

import jax
import jax.numpy as jnp
from jax import lax
from jax.experimental import pallas as pl
from jax.experimental.pallas import tpu as pltpu
from jax.sharding import Mesh, PartitionSpec as P


F32 = jnp.float32
BF16 = jnp.bfloat16
ALL = ("space", "high", "low")
MOST = ("space", "high")
LANES = 128
BLOCK = 1024
SUB = 512
WINDOW_ROWS = 32
VMEM = 16 * 1024 * 1024
EDGE_VMEM = 60 * 1024 * 1024


def sliced(width, parts):
    return width % (16 * parts) == 0


def cost(flops, nbytes):
    return pl.CostEstimate(flops=flops, bytes_accessed=nbytes, transcendentals=0)


def mix(a, b, left, right):
    return lax.dot_general(a, b, (((left,), (right,)), ((), ())), preferred_element_type=F32)


def full(array):
    return pl.BlockSpec(array.shape, lambda *_: (0,) * array.ndim)


def rows_of(line, count):
    return [line[:, j * LANES : (j + 1) * LANES] for j in range(count)]


def columns_of(lines):
    used = jnp.concatenate([line.astype(F32) for line in lines], axis=0)
    pad = jnp.zeros((LANES - used.shape[0], LANES), F32)
    turned = jnp.concatenate([used, pad], axis=0).T
    return [turned[:, j : j + 1] for j in range(len(lines))]


def one_hot_rows(columns, width, base=0.0):
    lane = lax.broadcasted_iota(jnp.int32, (LANES, width), 1).astype(F32)
    hot = [jnp.where(lane == column, 1.0, base).astype(BF16) for column in columns]
    return jnp.concatenate(hot, axis=0)


def one_hot_cols(lines, height):
    row = lax.broadcasted_iota(jnp.int32, (height, LANES), 0)
    hot = [jnp.where(row == line, 1.0, 0.0).astype(BF16) for line in lines]
    return jnp.concatenate(hot, axis=1)


def table_rows(sender, mesh_rows, band, shards):
    window = lax.div(sender, mesh_rows)
    target = band + window - 1
    window = jnp.where((target >= 0) & (target < shards), window, 1)
    return window * mesh_rows + lax.rem(sender, mesh_rows)


def groups(x):
    return jnp.sum(x.reshape(x.shape[0] // 8, 8, x.shape[1]), axis=0)


def split(x):
    hi = x.astype(BF16)
    return hi, (x - hi.astype(F32)).astype(BF16)


def store_pieces(out_ref, base, total):
    parts = out_ref.shape[0]
    own = total.shape[0] // parts
    for j, piece in enumerate(tiles_of(total)):
        at = pl.ds(base + j * own, own)
        out_ref[:, at, :] = piece.astype(BF16).reshape(parts, own, LANES)


def tiles_of(rows):
    return [rows[:, j : j + LANES] for j in range(0, rows.shape[1], LANES)]


def edge_kernel(
    shards, mesh_rows, halved,
    place_ref, send_ref, recv_ref, live_ref, grid_ref, cot_ref, lat_ref, pair_ref, other_ref,
    wsend_ref, wrecv_ref, wout_ref, bias_ref, gain_ref,
    dsend_ref, dkeep_ref, gsend_ref, gkeep_ref, own_ref, up_ref, down_ref,
    rows_tab, cot_tab, wsum, gacc, tacc, qacc, total,
):
    step = pl.program_id(0)
    band, high, low = place_ref[0], place_ref[1], place_ref[2]
    even = lax.rem(band, 2) == 0
    height, width = grid_ref.shape
    first_bias = 3 * mesh_rows

    @pl.when(step == 0)
    def _():
        proj = jnp.dot(grid_ref[...], wrecv_ref[...], preferred_element_type=F32)
        rows_tab[:height, :] = (0.5 * proj).astype(BF16)
        pair = pair_ref[...].astype(F32)
        other = other_ref[...].astype(F32)
        rows = [jnp.where(even, other, pair), lat_ref[...].astype(F32), jnp.where(even, pair, other)]
        rows.append(jnp.zeros((WINDOW_ROWS - first_bias, width), F32))
        rows = jnp.concatenate(rows, axis=0).astype(BF16)
        sent = 0.5 * jnp.dot(rows, wsend_ref[...], preferred_element_type=F32)
        hi, lo = split(0.5 * bias_ref[...])
        row = lax.broadcasted_iota(jnp.int32, (WINDOW_ROWS, 1), 0)
        sent = jnp.where(row == first_bias, hi.astype(F32), sent)
        sent = jnp.where(row == first_bias + 1, lo.astype(F32), sent)
        rows_tab[height:, :] = jnp.concatenate(
            [sent, jnp.zeros((LANES - WINDOW_ROWS, width), F32)], axis=0
        ).astype(BF16)
        cot_tab[...] = (cot_ref[...].astype(F32) * gain_ref[...]).astype(BF16)
        for ref in (wsum, gacc, tacc, qacc):
            ref[...] = jnp.zeros_like(ref)

    pieces = BLOCK // LANES
    each = SUB // LANES
    near = table_rows(send_ref[...], mesh_rows, band, shards)
    near_lines = rows_of(near, pieces)
    recv_lines = rows_of(recv_ref[...], pieces)
    cols = columns_of(recv_lines + near_lines + rows_of(live_ref[...], pieces))
    lane = lax.broadcasted_iota(jnp.int32, (1, LANES), 1)
    always = jnp.where((lane == first_bias) | (lane == first_bias + 1), 1.0, 0.0)
    scale = 1.0 / width
    for part in range(BLOCK // SUB):
        span = range(part * each, (part + 1) * each)
        hot = one_hot_rows([cols[i] for i in span], height)
        hot_near = one_hot_rows([cols[pieces + i] for i in span], LANES, always)
        live = jnp.concatenate([cols[2 * pieces + i] for i in span], axis=0)
        z = jnp.dot(
            jnp.concatenate([hot, hot_near], axis=1), rows_tab[...], preferred_element_type=F32
        )
        scaled = jnp.dot(hot, cot_tab[...], preferred_element_type=F32)
        t = jnp.tanh(z)
        u = t + 1.0
        h = z * u
        hidden = h.astype(BF16)
        slope = u + h * (1.0 - t)
        outer = jnp.dot(hidden, wout_ref[...], preferred_element_type=F32)
        center = outer - jnp.sum(outer, axis=-1, keepdims=True) * scale
        var = jnp.sum(center * center, axis=-1, keepdims=True) * scale
        inv = lax.rsqrt(var + 1e-05) * live
        normed = center * inv
        product = scaled * normed
        mean_s = jnp.sum(scaled, axis=-1, keepdims=True) * scale
        mean_sn = jnp.sum(product, axis=-1, keepdims=True) * scale
        d_outer = ((scaled - mean_s - normed * mean_sn) * inv).astype(BF16)
        qacc[...] += groups(product)
        wsum[...] += mix(hidden, d_outer, 0, 0)
        d_pre = (mix(d_outer, wout_ref[...], 1, 1) * slope).astype(BF16)
        hot = one_hot_cols([recv_lines[i] for i in span], height)
        gacc[...] += jnp.dot(hot, d_pre, preferred_element_type=F32)
        hot = one_hot_cols([near_lines[i] for i in span], WINDOW_ROWS)
        tacc[...] += jnp.dot(hot, d_pre, preferred_element_type=F32)

    @pl.when(step == pl.num_programs(0) - 1)
    def _():
        below = 0.5 * tacc[:mesh_rows, :]
        above = 0.5 * tacc[2 * mesh_rows : 3 * mesh_rows, :]
        own_ref[...] = 0.5 * tacc[mesh_rows : 2 * mesh_rows, :]
        up_ref[...] = jnp.where(even, above, below)
        edge = (band == 0) | (band == shards - 1)
        down_ref[...] = jnp.where(edge, 0.0, jnp.where(even, below, above))
        bias = 0.5 * jnp.sum(tacc[...], axis=0, keepdims=True)
        gain = jnp.sum(qacc[...], axis=0, keepdims=True) / gain_ref[...]
        gacc[...] = 0.5 * gacc[...]
        total[...] = mix(grid_ref[...], gacc[...].astype(BF16), 0, 0)
        half = (dkeep_ref.shape[0] - 8) // 2
        mine = pl.multiple_of(low * half, half) if halved else 0
        for k, whole in enumerate((wsum, total)):
            dkeep_ref[k * half : (k + 1) * half, :] = whole[pl.ds(mine, half), :]
            if halved:
                theirs = pl.multiple_of((1 - low) * half, half)
                dsend_ref[k * half : (k + 1) * half, :] = whole[pl.ds(theirs, half), :].astype(BF16)
        rest = jnp.zeros((4, width), F32)
        dkeep_ref[2 * half :, :] = jnp.concatenate([bias, gain, rest[:2], rest], axis=0)
        (bias_hi, bias_lo), (gain_hi, gain_lo) = split(bias), split(gain)
        sent = [v.astype(F32) for v in (bias_hi, gain_hi, bias_lo, gain_lo)]
        dsend_ref[dsend_ref.shape[0] - 8 :, :] = jnp.concatenate(sent + [rest], axis=0).astype(BF16)
        share = gkeep_ref.shape[1]
        for k in range(gkeep_ref.shape[0]):
            base = (high ^ k) * 2
            mine = pl.multiple_of((base + low) * share, share)
            theirs = pl.multiple_of((base + 1 - low) * share, share)
            gkeep_ref[k] = gacc[pl.ds(mine, share), :]
            gsend_ref[k] = gacc[pl.ds(theirs, share), :].astype(BF16)


def edges(shards, levels, place, send, recv, live, grid, cot, lat, pair, other, *weights):
    slots = send.shape[1]
    height, width = grid.shape
    mesh_rows = lat.shape[0]
    halved = sliced(width, shards * levels)
    line = pl.BlockSpec((1, BLOCK), lambda i: (0, i))
    half = width // 2 if halved else width
    share = (levels // 2, height // levels, width)
    near = jax.ShapeDtypeStruct((mesh_rows, width), F32)
    outs = [
        jax.ShapeDtypeStruct(((width if halved else 0) + 8, width), BF16),
        jax.ShapeDtypeStruct((2 * half + 8, width), F32),
        jax.ShapeDtypeStruct(share, BF16),
        jax.ShapeDtypeStruct(share, F32),
        near, near, near,
    ]
    whole = (grid, cot, lat, pair, other) + weights
    return pl.pallas_call(
        functools.partial(edge_kernel, shards, mesh_rows, halved),
        grid=(slots // BLOCK,),
        in_specs=[pl.BlockSpec(memory_space=pltpu.SMEM), line, line, line]
        + [full(array) for array in whole],
        out_specs=[full(out) for out in outs],
        out_shape=outs,
        scratch_shapes=[
            pltpu.VMEM((height + LANES, width), BF16),
            pltpu.VMEM((height, width), BF16),
            pltpu.VMEM((width, width), F32),
            pltpu.VMEM((height, width), F32),
            pltpu.VMEM((WINDOW_ROWS, width), F32),
            pltpu.VMEM((8, width), F32),
            pltpu.VMEM((width, width), F32),
        ],
        compiler_params=pltpu.CompilerParams(vmem_limit_bytes=EDGE_VMEM),
        cost_estimate=cost(14 * slots * width * width, 16 * width * width),
        name="edges",
    )(place, send, recv, live, *whole)


def combine_kernel(dkeep_ref, drecv_ref, gkeep_ref, grecv_ref, part_ref, gsend_ref, gown_ref):
    half = (dkeep_ref.shape[0] - 8) // 2
    width = dkeep_ref.shape[1]
    slab = half * width // LANES // part_ref.shape[0]
    for k in range(2):
        at = pl.ds(k * half, half)
        store_pieces(part_ref, k * slab, dkeep_ref[at, :] + drecv_ref[at, :].astype(F32))
    near = drecv_ref[2 * half :, :].astype(F32)
    vectors = dkeep_ref[2 * half : 2 * half + 2, :] + near[0:2] + near[2:4]
    hi, lo = split(vectors)
    extra = [v[k : k + 1] for v in (hi.astype(F32), lo.astype(F32)) for k in range(2)]
    extra = jnp.concatenate([tile for v in extra for tile in tiles_of(v)], axis=0).astype(BF16)
    part_ref[:, 2 * slab :, :] = jnp.broadcast_to(extra[None], (part_ref.shape[0],) + extra.shape)
    gown_ref[...] = gkeep_ref[0] + grecv_ref[0].astype(F32)
    gsend_ref[...] = (gkeep_ref[1] + grecv_ref[1].astype(F32)).astype(BF16)


def combine(parts, dkeep, drecv, gkeep, grecv):
    half, width = (dkeep.shape[0] - 8) // 2, dkeep.shape[1]
    rows = (2 * half // parts + 4) * (width // LANES)
    return pl.pallas_call(
        combine_kernel,
        out_shape=[
            jax.ShapeDtypeStruct((parts, rows, LANES), BF16),
            jax.ShapeDtypeStruct(gkeep.shape[1:], BF16),
            jax.ShapeDtypeStruct(gkeep.shape[1:], F32),
        ],
        compiler_params=pltpu.CompilerParams(vmem_limit_bytes=EDGE_VMEM),
        cost_estimate=cost(2 * dkeep.size, 8 * dkeep.size),
        name="combine_halves",
    )(dkeep, drecv, gkeep, grecv)


def sum_kernel(
    part_ref, lat_ref, own_ref, pair_ref, other_ref, wsend_ref,
    pay_ref, dmesh_ref, dbias_ref, dgain_ref,
):
    tiles = dbias_ref.shape[1] // LANES
    slabs = part_ref.shape[1] - 4 * tiles
    total = jnp.sum(part_ref[...].astype(F32), axis=0)
    for k, ref in enumerate((dbias_ref, dgain_ref)):
        base = slabs + k * tiles
        both = total[base : base + tiles] + total[base + 2 * tiles : base + 3 * tiles]
        for j in range(tiles):
            ref[:, j * LANES : (j + 1) * LANES] = both[j : j + 1]
    mesh = own_ref[...] + pair_ref[...] + other_ref[...]
    pieces = [total[:slabs]] + tiles_of(mesh) + tiles_of(lat_ref[...].astype(F32))
    payload = jnp.concatenate(pieces, axis=0).astype(BF16)
    pay_ref[...] = jnp.broadcast_to(payload[None], pay_ref.shape)
    dmesh_ref[...] = mix(mesh.astype(BF16), wsend_ref[...], 1, 1)


def sum_slabs(shards, part, lat, own, pair, other, wsend):
    mesh_rows, width = lat.shape
    tiles = width // LANES
    rows = part.shape[1] - 4 * tiles + 2 * mesh_rows * tiles
    vector = jax.ShapeDtypeStruct((1, width), F32)
    return pl.pallas_call(
        sum_kernel,
        out_shape=[
            jax.ShapeDtypeStruct((shards, rows, LANES), BF16),
            jax.ShapeDtypeStruct((mesh_rows, width), F32),
            vector, vector,
        ],
        compiler_params=pltpu.CompilerParams(vmem_limit_bytes=VMEM),
        cost_estimate=cost(2 * part.size, 4 * part.size),
        name="sum_slabs",
    )(part, lat, own, pair, other, wsend)


def spread_kernel(levels, mesh_rows, place_ref, *refs):
    parts_refs = refs[:levels]
    dsend_ref, drecv_ref, dout_ref, mesh, lat = refs[levels:]
    width = dsend_ref.shape[0]
    tiles = width // LANES
    shards = parts_refs[0].shape[0]
    own = width // (shards * levels)
    slab = own * tiles
    level = place_ref[1] * 2 + place_ref[2]
    for k, ref in enumerate(parts_refs):
        for s in range(shards):
            at = level ^ k
            high, low = lax.shift_right_logical(at, 1), at & 1
            place = (low * shards + s) * (levels // 2) + high
            tail = ref[s, 2 * slab :, :].astype(F32)
            rows = pl.ds(pl.multiple_of(place * own, own), own)
            near = pl.ds(pl.multiple_of(place * mesh_rows, mesh_rows), mesh_rows)
            for j in range(tiles):
                cols = pl.ds(j * LANES, LANES)
                dout_ref[rows, cols] = ref[s, j * own : (j + 1) * own, :]
                drecv_ref[rows, cols] = ref[s, slab + j * own : slab + (j + 1) * own, :]
                mesh[near, cols] = tail[j * mesh_rows : (j + 1) * mesh_rows]
                lat[near, cols] = tail[(tiles + j) * mesh_rows : (tiles + j + 1) * mesh_rows]
    dsend_ref[...] = mix(lat[...].astype(BF16), mesh[...].astype(BF16), 0, 0).astype(BF16)


def spread(width, mesh_rows, place, received):
    levels = len(received)
    rows = received[0].shape[0] * levels * mesh_rows
    out = jax.ShapeDtypeStruct((width, width), BF16)
    return pl.pallas_call(
        functools.partial(spread_kernel, levels, mesh_rows),
        in_specs=[pl.BlockSpec(memory_space=pltpu.SMEM)]
        + [pl.BlockSpec(memory_space=pltpu.VMEM)] * levels,
        out_shape=[out, out, out],
        scratch_shapes=[pltpu.VMEM((rows, width), F32)] * 2,
        compiler_params=pltpu.CompilerParams(vmem_limit_bytes=VMEM),
        cost_estimate=cost(2 * rows * width * width, 8 * width * width),
        name="spread_weights",
    )(place, *received)


def swap(x, axis, bit):
    return lax.ppermute(x, axis, [(i, i ^ bit) for i in range(lax.axis_size(axis))])


def swap_between(x, axis):
    count = lax.axis_size(axis)
    pairs = [(i, i + 1) for i in range(1, count - 1, 2)]
    ends = [(0, 0), (count - 1, count - 1)]
    return lax.ppermute(x, axis, pairs + [(j, i) for i, j in pairs] + ends)


def body(
    grid_latent, mesh_latent, grid_output_cotangent, w_send, w_recv, output_weight,
    hidden_layer_bias, output_norm_gain, edge_sender, edge_receiver, edge_live,
):
    shards, levels = lax.axis_size("space"), lax.axis_size("high") * 2
    parts = shards * levels
    width = grid_latent.shape[1]
    mesh_rows = mesh_latent.shape[1]
    lat = mesh_latent[0]
    whole_slabs = sliced(width, parts)
    place = jnp.stack([lax.axis_index(axis) for axis in ALL]).astype(jnp.int32)

    lat_pair = swap(lat, "space", 1)
    lat_other = swap_between(lat, "space")
    dsend, dkeep, gsend, gkeep, own, pair, other = edges(
        shards, levels, place, edge_sender, edge_receiver, edge_live,
        grid_latent, grid_output_cotangent, lat, lat_pair, lat_other,
        w_send, w_recv, output_weight, hidden_layer_bias[None], output_norm_gain[None],
    )
    pair = swap(pair, "space", 1)
    other = swap_between(other, "space")

    if not whole_slabs:
        rows = jnp.stack([gkeep.astype(BF16), gsend])
        for k in range(1, levels):
            side = rows[k % 2, k // 2]
            for bit in (1, 2):
                if k & bit:
                    side = swap(side, ("low", "high")[bit // 2], 1)
            gkeep = gkeep.at[0].add(side.astype(F32))
        d_grid = mix(gkeep[0].astype(BF16), w_recv, 1, 1)
        mesh = (own + pair + other).astype(BF16)
        d_mesh = mix(mesh, w_send, 1, 1)
        d_send, rest = lax.psum((mix(lat, mesh, 0, 0), dkeep), ALL)
        d_w_out, d_w_recv = rest[:width].astype(BF16), rest[width : 2 * width].astype(BF16)
        d_bias, d_gain = rest[2 * width], rest[2 * width + 1]
        return (d_grid, d_mesh[None], d_send.astype(BF16), d_w_recv, d_w_out, d_bias, d_gain)

    dnear = swap(dsend, "low", 1)
    gnear = swap(gsend, "low", 1)
    part, gsend, gown = combine(parts // 2, dkeep, dnear, gkeep, gnear)
    gfar = swap(gsend, "high", 1)
    part = lax.all_to_all(part, MOST, 0, 0, tiled=False)
    d_grid = mix((gown + gfar.astype(F32)).astype(BF16), w_recv, 1, 1)
    payload, d_mesh, d_bias, d_gain = sum_slabs(shards, part, lat, own, pair, other, w_send)
    received = {0: lax.all_to_all(payload, "space", 0, 0, tiled=False)}
    received[2] = swap(received[0], "high", 1)
    received[1] = swap(received[0], "low", 1)
    received[3] = swap(received[2], "low", 1)
    d_w_send, d_w_recv, d_w_out = spread(
        width, mesh_rows, place, [received[k] for k in range(levels)]
    )
    return (d_grid, d_mesh[None], d_w_send, d_w_recv, d_w_out, d_bias[0], d_gain[0])


def solution(mesh):
    shards, levels = mesh.devices.shape
    split_mesh = Mesh(mesh.devices.reshape(shards, levels // 2, 2), ALL)
    level = MOST[1:] + ALL[2:]

    return jax.shard_map(
        body,
        mesh=split_mesh,
        in_specs=(
            P("space", None), P(level, "space", None), P("space", None), P(), P(), P(), P(), P(),
            P(level, "space"), P(level, "space"), P(level, "space"),
        ),
        out_specs=(P(ALL, None), P(level, "space", None), P(), P(), P(), P(), P()),
        check_vma=False,
    )
```

```python
import functools

import jax
import jax.numpy as jnp
from jax import lax
from jax.experimental import pallas as pl
from jax.experimental.pallas import tpu as pltpu
from jax.sharding import Mesh, PartitionSpec as P


F32 = jnp.float32
BF16 = jnp.bfloat16
ALL = ("space", "high", "low")
MOST = ("space", "high")
LANES = 128
BLOCK = 2048
SUB = 256
WINDOW_ROWS = 32
VMEM = 16 * 1024 * 1024
EDGE_VMEM = 40 * 1024 * 1024
COMBINE_VMEM = 16 * 1024 * 1024


def sliced(width, parts):
    return width % (16 * parts) == 0


def cost(flops, nbytes):
    return pl.CostEstimate(flops=flops, bytes_accessed=nbytes, transcendentals=0)


def mix(a, b, left, right):
    return lax.dot_general(a, b, (((left,), (right,)), ((), ())), preferred_element_type=F32)


def full(array):
    return pl.BlockSpec(array.shape, lambda *_: (0,) * array.ndim)


def rows_of(line, count):
    return [line[:, j * LANES : (j + 1) * LANES] for j in range(count)]


def columns_of(lines):
    used = jnp.concatenate([line.astype(F32) for line in lines], axis=0)
    pad = jnp.zeros((LANES - used.shape[0], LANES), F32)
    turned = jnp.concatenate([used, pad], axis=0).T
    return [turned[:, j : j + 1] for j in range(len(lines))]


def one_hot_rows(columns, width, base=0.0):
    lane = lax.broadcasted_iota(jnp.int32, (LANES, width), 1).astype(F32)
    hot = [jnp.where(lane == column, 1.0, base).astype(BF16) for column in columns]
    return jnp.concatenate(hot, axis=0)


def one_hot_cols(lines, height):
    row = lax.broadcasted_iota(jnp.int32, (height, LANES), 0)
    hot = [jnp.where(row == line, 1.0, 0.0).astype(BF16) for line in lines]
    return jnp.concatenate(hot, axis=1)


def table_rows(sender, mesh_rows, band, shards):
    window = lax.div(sender, mesh_rows)
    target = band + window - 1
    window = jnp.where((target >= 0) & (target < shards), window, 1)
    return window * mesh_rows + lax.rem(sender, mesh_rows)


def groups(x):
    return jnp.sum(x.reshape(x.shape[0] // 8, 8, x.shape[1]), axis=0)


def split(x):
    hi = x.astype(BF16)
    return hi, (x - hi.astype(F32)).astype(BF16)


def store_pieces(out_ref, base, total):
    parts = out_ref.shape[0]
    own = total.shape[0] // parts
    for j, piece in enumerate(tiles_of(total)):
        at = pl.ds(base + j * own, own)
        out_ref[:, at, :] = piece.astype(BF16).reshape(parts, own, LANES)


def tiles_of(rows):
    return [rows[:, j : j + LANES] for j in range(0, rows.shape[1], LANES)]


def edge_kernel(shards, mesh_rows, halved, fetched, place_ref, pair_ref, other_ref, *refs):
    sources, refs = refs[:fetched], refs[fetched:]
    dsend_ref, dkeep_ref, gsend_ref, gkeep_ref, own_ref, up_ref, down_ref = refs[:7]
    copies, refs = refs[7 : 7 + fetched], refs[7 + fetched :]
    rows_tab, cot_tab, wsum, gacc, tacc, qacc, total, sems = refs
    grid_ref, wrecv_ref, lat_ref, wsend_ref, bias_ref, gain_ref, cot_ref = copies[:7]
    send_ref, recv_ref, live_ref, wout_ref = copies[7:]
    step = pl.program_id(0)
    band, high, low = place_ref[0], place_ref[1], place_ref[2]
    even = lax.rem(band, 2) == 0
    height, width = grid_ref.shape
    first_bias = 3 * mesh_rows

    def fetch(k):
        return pltpu.make_async_copy(sources[k], copies[k], sems.at[k])

    @pl.when(step == 0)
    def _():
        for k in range(fetched):
            fetch(k).start()

    def arrived(first, last):
        for k in range(first, last):
            fetch(k).wait()

    @pl.when(step == 0)
    def _():
        for ref in (wsum, gacc, tacc, qacc):
            ref[...] = jnp.zeros_like(ref)
        arrived(0, 2)
        proj = jnp.dot(grid_ref[...], wrecv_ref[...], preferred_element_type=F32)
        rows_tab[:height, :] = (0.5 * proj).astype(BF16)
        arrived(2, 5)
        pair = pair_ref[...].astype(F32)
        other = other_ref[...].astype(F32)
        rows = [jnp.where(even, other, pair), lat_ref[...].astype(F32), jnp.where(even, pair, other)]
        rows.append(jnp.zeros((WINDOW_ROWS - first_bias, width), F32))
        rows = jnp.concatenate(rows, axis=0).astype(BF16)
        sent = 0.5 * jnp.dot(rows, wsend_ref[...], preferred_element_type=F32)
        hi, lo = split(0.5 * bias_ref[...])
        row = lax.broadcasted_iota(jnp.int32, (WINDOW_ROWS, 1), 0)
        sent = jnp.where(row == first_bias, hi.astype(F32), sent)
        sent = jnp.where(row == first_bias + 1, lo.astype(F32), sent)
        rows_tab[height:, :] = jnp.concatenate(
            [sent, jnp.zeros((LANES - WINDOW_ROWS, width), F32)], axis=0
        ).astype(BF16)
        arrived(5, 7)
        cot_tab[...] = (cot_ref[...].astype(F32) * gain_ref[...]).astype(BF16)
        arrived(7, fetched)

    pieces = BLOCK // LANES
    each = SUB // LANES
    block = pl.ds(pl.multiple_of(step * BLOCK, BLOCK), BLOCK)
    near = table_rows(send_ref[:, block], mesh_rows, band, shards)
    near_lines = rows_of(near, pieces)
    recv_lines = rows_of(recv_ref[:, block], pieces)
    cols = columns_of(recv_lines + near_lines + rows_of(live_ref[:, block], pieces))
    lane = lax.broadcasted_iota(jnp.int32, (1, LANES), 1)
    always = jnp.where((lane == first_bias) | (lane == first_bias + 1), 1.0, 0.0)
    scale = 1.0 / width
    count = BLOCK // SUB
    spans = [range(part * each, (part + 1) * each) for part in range(count)]

    def hot_rows(span):
        hot = one_hot_rows([cols[i] for i in span], height)
        near = one_hot_rows([cols[pieces + i] for i in span], LANES, always)
        return hot, jnp.concatenate([hot, near], axis=1)

    def row_mean(x):
        return jnp.sum(x, axis=-1, keepdims=True) * scale

    ahead, behind = hot_rows(spans[0]), None
    for part in range(count + 1):
        if part < count:
            z = jnp.dot(ahead[1], rows_tab[...], preferred_element_type=F32)
            scaled = jnp.dot(ahead[0], cot_tab[...], preferred_element_type=F32)
        if behind is not None:
            span, hidden_b, slope_b, scaled_b, outer = behind
            live = jnp.concatenate([cols[2 * pieces + i] for i in span], axis=0)
            center = outer - row_mean(outer)
            inv = lax.rsqrt(row_mean(center * center) + 1e-05) * live
            normed = center * inv
            product = scaled_b * normed
            d_outer = scaled_b - row_mean(scaled_b) - normed * row_mean(product)
            d_outer = (d_outer * inv).astype(BF16)
            qacc[...] += groups(product)
            wsum[...] += mix(hidden_b, d_outer, 0, 0)
            d_hidden = mix(d_outer, wout_ref[...], 1, 1)
        if part < count:
            t = jnp.tanh(z)
            u = t + 1.0
            h = z * u
            hidden = h.astype(BF16)
            slope = u + h * (1.0 - t)
            outer = jnp.dot(hidden, wout_ref[...], preferred_element_type=F32)
        if behind is not None:
            d_pre = (d_hidden * slope_b).astype(BF16)
            hot = one_hot_cols([recv_lines[i] for i in span], height)
            gacc[...] += jnp.dot(hot, d_pre, preferred_element_type=F32)
            hot = one_hot_cols([near_lines[i] for i in span], WINDOW_ROWS)
            tacc[...] += jnp.dot(hot, d_pre, preferred_element_type=F32)
        if part < count:
            behind = (spans[part], hidden, slope, scaled, outer)
        if part + 1 < count:
            ahead = hot_rows(spans[part + 1])

    @pl.when(step == pl.num_programs(0) - 1)
    def _():
        below = 0.5 * tacc[:mesh_rows, :]
        above = 0.5 * tacc[2 * mesh_rows : 3 * mesh_rows, :]
        own_ref[...] = 0.5 * tacc[mesh_rows : 2 * mesh_rows, :]
        up_ref[...] = jnp.where(even, above, below)
        edge = (band == 0) | (band == shards - 1)
        down_ref[...] = jnp.where(edge, 0.0, jnp.where(even, below, above))
        bias = 0.5 * jnp.sum(tacc[...], axis=0, keepdims=True)
        gain = jnp.sum(qacc[...], axis=0, keepdims=True) / gain_ref[...]
        gacc[...] = 0.5 * gacc[...]
        total[...] = mix(grid_ref[...], gacc[...].astype(BF16), 0, 0)
        half = (dkeep_ref.shape[0] - 8) // 2
        mine = pl.multiple_of(low * half, half) if halved else 0
        for k, whole in enumerate((wsum, total)):
            dkeep_ref[k * half : (k + 1) * half, :] = whole[pl.ds(mine, half), :]
            if halved:
                theirs = pl.multiple_of((1 - low) * half, half)
                dsend_ref[k * half : (k + 1) * half, :] = whole[pl.ds(theirs, half), :].astype(BF16)
        rest = jnp.zeros((4, width), F32)
        dkeep_ref[2 * half :, :] = jnp.concatenate([bias, gain, rest[:2], rest], axis=0)
        (bias_hi, bias_lo), (gain_hi, gain_lo) = split(bias), split(gain)
        sent = [v.astype(F32) for v in (bias_hi, gain_hi, bias_lo, gain_lo)]
        dsend_ref[dsend_ref.shape[0] - 8 :, :] = jnp.concatenate(sent + [rest], axis=0).astype(BF16)
        share = gkeep_ref.shape[1]
        for k in range(gkeep_ref.shape[0]):
            base = (high ^ k) * 2
            mine = pl.multiple_of((base + low) * share, share)
            theirs = pl.multiple_of((base + 1 - low) * share, share)
            gkeep_ref[k] = gacc[pl.ds(mine, share), :]
            gsend_ref[k] = gacc[pl.ds(theirs, share), :].astype(BF16)


def edges(shards, levels, place, pair, other, *fetched):
    grid, send = fetched[0], fetched[7]
    slots = send.shape[1]
    height, width = grid.shape
    mesh_rows = pair.shape[0]
    halved = sliced(width, shards * levels)
    half = width // 2 if halved else width
    share = (levels // 2, height // levels, width)
    near = jax.ShapeDtypeStruct((mesh_rows, width), F32)
    outs = [
        jax.ShapeDtypeStruct(((width if halved else 0) + 8, width), BF16),
        jax.ShapeDtypeStruct((2 * half + 8, width), F32),
        jax.ShapeDtypeStruct(share, BF16),
        jax.ShapeDtypeStruct(share, F32),
        near, near, near,
    ]
    return pl.pallas_call(
        functools.partial(edge_kernel, shards, mesh_rows, halved, len(fetched)),
        grid=(slots // BLOCK,),
        in_specs=[pl.BlockSpec(memory_space=pltpu.SMEM), full(pair), full(other)]
        + [pl.BlockSpec(memory_space=pltpu.HBM)] * len(fetched),
        out_specs=[full(out) for out in outs],
        out_shape=outs,
        scratch_shapes=[pltpu.VMEM(array.shape, array.dtype) for array in fetched]
        + [
            pltpu.VMEM((height + LANES, width), BF16),
            pltpu.VMEM((height, width), BF16),
            pltpu.VMEM((width, width), F32),
            pltpu.VMEM((height, width), F32),
            pltpu.VMEM((WINDOW_ROWS, width), F32),
            pltpu.VMEM((8, width), F32),
            pltpu.VMEM((width, width), F32),
            pltpu.SemaphoreType.DMA((len(fetched),)),
        ],
        compiler_params=pltpu.CompilerParams(vmem_limit_bytes=EDGE_VMEM),
        cost_estimate=cost(14 * slots * width * width, 16 * width * width),
        name="edges",
    )(place, pair, other, *[pltpu.with_memory_space_constraint(x, pltpu.HBM) for x in fetched])


def combine_kernel(dkeep_ref, drecv_ref, gkeep_ref, grecv_ref, part_ref, gsend_ref, gown_ref):
    half = (dkeep_ref.shape[0] - 8) // 2
    width = dkeep_ref.shape[1]
    slab = half * width // LANES // part_ref.shape[0]
    for k in range(2):
        at = pl.ds(k * half, half)
        store_pieces(part_ref, k * slab, dkeep_ref[at, :] + drecv_ref[at, :].astype(F32))
    near = drecv_ref[2 * half :, :].astype(F32)
    vectors = dkeep_ref[2 * half : 2 * half + 2, :] + near[0:2] + near[2:4]
    hi, lo = split(vectors)
    extra = [v[k : k + 1] for v in (hi.astype(F32), lo.astype(F32)) for k in range(2)]
    extra = jnp.concatenate([tile for v in extra for tile in tiles_of(v)], axis=0).astype(BF16)
    part_ref[:, 2 * slab :, :] = jnp.broadcast_to(extra[None], (part_ref.shape[0],) + extra.shape)
    gown_ref[...] = gkeep_ref[0] + grecv_ref[0].astype(F32)
    gsend_ref[...] = (gkeep_ref[1] + grecv_ref[1].astype(F32)).astype(BF16)


def combine(parts, dkeep, drecv, gkeep, grecv):
    half, width = (dkeep.shape[0] - 8) // 2, dkeep.shape[1]
    rows = (2 * half // parts + 4) * (width // LANES)
    return pl.pallas_call(
        combine_kernel,
        out_shape=[
            jax.ShapeDtypeStruct((parts, rows, LANES), BF16),
            jax.ShapeDtypeStruct(gkeep.shape[1:], BF16),
            jax.ShapeDtypeStruct(gkeep.shape[1:], F32),
        ],
        compiler_params=pltpu.CompilerParams(vmem_limit_bytes=COMBINE_VMEM),
        cost_estimate=cost(2 * dkeep.size, 8 * dkeep.size),
        name="combine_halves",
    )(dkeep, drecv, gkeep, grecv)


def sum_kernel(
    part_ref, lat_ref, own_ref, pair_ref, other_ref, wsend_ref,
    pay_ref, dmesh_ref, dbias_ref, dgain_ref,
):
    tiles = dbias_ref.shape[1] // LANES
    slabs = part_ref.shape[1] - 4 * tiles
    total = jnp.sum(part_ref[...].astype(F32), axis=0)
    for k, ref in enumerate((dbias_ref, dgain_ref)):
        base = slabs + k * tiles
        both = total[base : base + tiles] + total[base + 2 * tiles : base + 3 * tiles]
        for j in range(tiles):
            ref[:, j * LANES : (j + 1) * LANES] = both[j : j + 1]
    mesh = own_ref[...] + pair_ref[...] + other_ref[...]
    pieces = [total[:slabs]] + tiles_of(mesh) + tiles_of(lat_ref[...].astype(F32))
    payload = jnp.concatenate(pieces, axis=0).astype(BF16)
    pay_ref[...] = jnp.broadcast_to(payload[None], pay_ref.shape)
    dmesh_ref[...] = mix(mesh.astype(BF16), wsend_ref[...], 1, 1)


def sum_slabs(shards, part, lat, own, pair, other, wsend):
    mesh_rows, width = lat.shape
    tiles = width // LANES
    rows = part.shape[1] - 4 * tiles + 2 * mesh_rows * tiles
    vector = jax.ShapeDtypeStruct((1, width), F32)
    return pl.pallas_call(
        sum_kernel,
        out_shape=[
            jax.ShapeDtypeStruct((shards, rows, LANES), BF16),
            jax.ShapeDtypeStruct((mesh_rows, width), F32),
            vector, vector,
        ],
        compiler_params=pltpu.CompilerParams(vmem_limit_bytes=VMEM),
        cost_estimate=cost(2 * part.size, 4 * part.size),
        name="sum_slabs",
    )(part, lat, own, pair, other, wsend)


def spread_kernel(levels, mesh_rows, place_ref, *refs):
    parts_refs = refs[:levels]
    dsend_ref, drecv_ref, dout_ref, mesh, lat = refs[levels:]
    width = dsend_ref.shape[0]
    tiles = width // LANES
    shards = parts_refs[0].shape[0]
    own = width // (shards * levels)
    slab = own * tiles
    level = place_ref[1] * 2 + place_ref[2]
    for k, ref in enumerate(parts_refs):
        for s in range(shards):
            at = level ^ k
            high, low = lax.shift_right_logical(at, 1), at & 1
            place = (low * shards + s) * (levels // 2) + high
            tail = ref[s, 2 * slab :, :].astype(F32)
            rows = pl.ds(pl.multiple_of(place * own, own), own)
            near = pl.ds(pl.multiple_of(place * mesh_rows, mesh_rows), mesh_rows)
            for j in range(tiles):
                cols = pl.ds(j * LANES, LANES)
                dout_ref[rows, cols] = ref[s, j * own : (j + 1) * own, :]
                drecv_ref[rows, cols] = ref[s, slab + j * own : slab + (j + 1) * own, :]
                mesh[near, cols] = tail[j * mesh_rows : (j + 1) * mesh_rows]
                lat[near, cols] = tail[(tiles + j) * mesh_rows : (tiles + j + 1) * mesh_rows]
    dsend_ref[...] = mix(lat[...].astype(BF16), mesh[...].astype(BF16), 0, 0).astype(BF16)


def spread(width, mesh_rows, place, received):
    levels = len(received)
    rows = received[0].shape[0] * levels * mesh_rows
    out = jax.ShapeDtypeStruct((width, width), BF16)
    return pl.pallas_call(
        functools.partial(spread_kernel, levels, mesh_rows),
        in_specs=[pl.BlockSpec(memory_space=pltpu.SMEM)]
        + [pl.BlockSpec(memory_space=pltpu.VMEM)] * levels,
        out_shape=[out, out, out],
        scratch_shapes=[pltpu.VMEM((rows, width), F32)] * 2,
        compiler_params=pltpu.CompilerParams(vmem_limit_bytes=VMEM),
        cost_estimate=cost(2 * rows * width * width, 8 * width * width),
        name="spread_weights",
    )(place, *received)


def swap(x, axis, bit):
    return lax.ppermute(x, axis, [(i, i ^ bit) for i in range(lax.axis_size(axis))])


def swap_between(x, axis):
    count = lax.axis_size(axis)
    pairs = [(i, i + 1) for i in range(1, count - 1, 2)]
    ends = [(0, 0), (count - 1, count - 1)]
    return lax.ppermute(x, axis, pairs + [(j, i) for i, j in pairs] + ends)


def body(
    grid_latent, mesh_latent, grid_output_cotangent, w_send, w_recv, output_weight,
    hidden_layer_bias, output_norm_gain, edge_sender, edge_receiver, edge_live,
):
    shards, levels = lax.axis_size("space"), lax.axis_size("high") * 2
    parts = shards * levels
    width = grid_latent.shape[1]
    mesh_rows = mesh_latent.shape[1]
    lat = mesh_latent[0]
    whole_slabs = sliced(width, parts)
    place = jnp.stack([lax.axis_index(axis) for axis in ALL]).astype(jnp.int32)

    lat_pair = swap(lat, "space", 1)
    lat_other = swap_between(lat, "space")
    dsend, dkeep, gsend, gkeep, own, pair, other = edges(
        shards, levels, place, lat_pair, lat_other,
        grid_latent, w_recv, lat, w_send, hidden_layer_bias[None], output_norm_gain[None],
        grid_output_cotangent, edge_sender, edge_receiver, edge_live, output_weight,
    )
    pair = swap(pair, "space", 1)
    other = swap_between(other, "space")

    if not whole_slabs:
        rows = jnp.stack([gkeep.astype(BF16), gsend])
        for k in range(1, levels):
            side = rows[k % 2, k // 2]
            for bit in (1, 2):
                if k & bit:
                    side = swap(side, ("low", "high")[bit // 2], 1)
            gkeep = gkeep.at[0].add(side.astype(F32))
        d_grid = mix(gkeep[0].astype(BF16), w_recv, 1, 1)
        mesh = (own + pair + other).astype(BF16)
        d_mesh = mix(mesh, w_send, 1, 1)
        d_send, rest = lax.psum((mix(lat, mesh, 0, 0), dkeep), ALL)
        d_w_out, d_w_recv = rest[:width].astype(BF16), rest[width : 2 * width].astype(BF16)
        d_bias, d_gain = rest[2 * width], rest[2 * width + 1]
        return (d_grid, d_mesh[None], d_send.astype(BF16), d_w_recv, d_w_out, d_bias, d_gain)

    dnear = swap(dsend, "low", 1)
    gnear = swap(gsend, "low", 1)
    part, gsend, gown = combine(parts // 2, dkeep, dnear, gkeep, gnear)
    gfar = swap(gsend, "high", 1)
    part = lax.all_to_all(part, MOST, 0, 0, tiled=False)
    d_grid = mix((gown + gfar.astype(F32)).astype(BF16), w_recv, 1, 1)
    payload, d_mesh, d_bias, d_gain = sum_slabs(shards, part, lat, own, pair, other, w_send)
    received = {0: lax.all_to_all(payload, "space", 0, 0, tiled=False)}
    received[2] = swap(received[0], "high", 1)
    received[1] = swap(received[0], "low", 1)
    received[3] = swap(received[2], "low", 1)
    d_w_send, d_w_recv, d_w_out = spread(
        width, mesh_rows, place, [received[k] for k in range(levels)]
    )
    return (d_grid, d_mesh[None], d_w_send, d_w_recv, d_w_out, d_bias[0], d_gain[0])


def solution(mesh):
    shards, levels = mesh.devices.shape
    split_mesh = Mesh(mesh.devices.reshape(shards, levels // 2, 2), ALL)
    level = MOST[1:] + ALL[2:]

    return jax.shard_map(
        body,
        mesh=split_mesh,
        in_specs=(
            P("space", None), P(level, "space", None), P("space", None), P(), P(), P(), P(), P(),
            P(level, "space"), P(level, "space"), P(level, "space"),
        ),
        out_specs=(P(ALL, None), P(level, "space", None), P(), P(), P(), P(), P()),
        check_vma=False,
    )
```

```python
import functools

import jax
import jax.numpy as jnp
from jax import lax
from jax.experimental import pallas as pl
from jax.experimental.pallas import tpu as pltpu
from jax.sharding import Mesh, PartitionSpec as P


F32 = jnp.float32
BF16 = jnp.bfloat16
ALL = ("space", "high", "low")
MOST = ("space", "high")
LANES = 128
BLOCK = 2048
SUB = 256
WINDOW_ROWS = 32
VMEM = 16 * 1024 * 1024
EDGE_VMEM = 40 * 1024 * 1024
COMBINE_VMEM = 16 * 1024 * 1024


def sliced(width, parts):
    return width % (16 * parts) == 0


def cost(flops, nbytes):
    return pl.CostEstimate(flops=flops, bytes_accessed=nbytes, transcendentals=0)


def mix(a, b, left, right):
    return lax.dot_general(a, b, (((left,), (right,)), ((), ())), preferred_element_type=F32)


def full(array):
    return pl.BlockSpec(array.shape, lambda *_: (0,) * array.ndim)


def rows_of(line, count):
    return [line[:, j * LANES : (j + 1) * LANES] for j in range(count)]


def columns_of(lines):
    used = jnp.concatenate([line.astype(F32) for line in lines], axis=0)
    pad = jnp.zeros((LANES - used.shape[0], LANES), F32)
    turned = jnp.concatenate([used, pad], axis=0).T
    return [turned[:, j : j + 1] for j in range(len(lines))]


def one_hot_rows(columns, width, base=0.0):
    lane = lax.broadcasted_iota(jnp.int32, (LANES, width), 1).astype(F32)
    hot = [jnp.where(lane == column, 1.0, base).astype(BF16) for column in columns]
    return jnp.concatenate(hot, axis=0)


def one_hot_cols(lines, height):
    row = lax.broadcasted_iota(jnp.int32, (height, LANES), 0)
    hot = [jnp.where(row == line, 1.0, 0.0).astype(BF16) for line in lines]
    return jnp.concatenate(hot, axis=1)


def table_rows(sender, mesh_rows, band, shards):
    window = lax.div(sender, mesh_rows)
    target = band + window - 1
    window = jnp.where((target >= 0) & (target < shards), window, 1)
    return window * mesh_rows + lax.rem(sender, mesh_rows)


def groups(x):
    return jnp.sum(x.reshape(x.shape[0] // 8, 8, x.shape[1]), axis=0)


def split(x):
    hi = x.astype(BF16)
    return hi, (x - hi.astype(F32)).astype(BF16)


def store_pieces(out_ref, base, total):
    parts = out_ref.shape[0]
    own = total.shape[0] // parts
    for j, piece in enumerate(tiles_of(total)):
        at = pl.ds(base + j * own, own)
        out_ref[:, at, :] = piece.astype(BF16).reshape(parts, own, LANES)


def tiles_of(rows):
    return [rows[:, j : j + LANES] for j in range(0, rows.shape[1], LANES)]


def table_kernel(fetched, *refs):
    sources, (rows_ref, cot_tab_ref) = refs[:fetched], refs[fetched : fetched + 2]
    copies, sems = refs[fetched + 2 : -1], refs[-1]
    grid_ref, w_ref, cot_ref, gain_ref = copies
    moves = [pltpu.make_async_copy(sources[k], copies[k], sems.at[k]) for k in range(fetched)]
    for move in moves:
        move.start()
    for move in moves[:2]:
        move.wait()
    proj = jnp.dot(grid_ref[...], w_ref[...], preferred_element_type=F32)
    rows_ref[...] = (0.5 * proj).astype(BF16)
    for move in moves[2:]:
        move.wait()
    cot_tab_ref[...] = (cot_ref[...].astype(F32) * gain_ref[...]).astype(BF16)


def tables(*fetched):
    out = jax.ShapeDtypeStruct(fetched[0].shape, BF16)
    return pl.pallas_call(
        functools.partial(table_kernel, len(fetched)),
        in_specs=[pl.BlockSpec(memory_space=pltpu.HBM)] * len(fetched),
        out_shape=[out, out],
        scratch_shapes=[pltpu.VMEM(array.shape, array.dtype) for array in fetched]
        + [pltpu.SemaphoreType.DMA((len(fetched),))],
        compiler_params=pltpu.CompilerParams(vmem_limit_bytes=VMEM),
        cost_estimate=cost(2 * out.size * out.shape[1], 4 * out.size),
        name="tables",
    )(*held(fetched))


def held(arrays):
    return [pltpu.with_memory_space_constraint(array, pltpu.HBM) for array in arrays]


def edge_kernel(shards, mesh_rows, halved, fetched, place_ref, pair_ref, other_ref, rows_ref, cot_tab, *refs):
    sources, refs = refs[:fetched], refs[fetched:]
    dsend_ref, dkeep_ref, gsend_ref, gkeep_ref, own_ref, up_ref, down_ref = refs[:7]
    copies, refs = refs[7 : 7 + fetched], refs[7 + fetched :]
    rows_tab, wsum, acc, qacc, total, sems = refs
    wsend_ref, lat_ref, bias_ref, send_ref, recv_ref, live_ref, wout_ref, gain_ref, grid_ref = copies
    step = pl.program_id(0)
    band, high, low = place_ref[0], place_ref[1], place_ref[2]
    even = lax.rem(band, 2) == 0
    height, width = grid_ref.shape
    gacc, tacc = acc.at[:height, :], acc.at[height:, :]
    first_bias = 3 * mesh_rows

    def fetch(k):
        return pltpu.make_async_copy(sources[k], copies[k], sems.at[k])

    @pl.when(step == 0)
    def _():
        for k in range(fetched):
            fetch(k).start()

    def arrived(first, last):
        for k in range(first, last):
            fetch(k).wait()

    @pl.when(step == 0)
    def _():
        for ref in (wsum, acc, qacc):
            ref[...] = jnp.zeros_like(ref)
        rows_tab[:height, :] = rows_ref[...]
        arrived(0, 3)
        pair = pair_ref[...].astype(F32)
        other = other_ref[...].astype(F32)
        rows = [jnp.where(even, other, pair), lat_ref[...].astype(F32), jnp.where(even, pair, other)]
        rows.append(jnp.zeros((WINDOW_ROWS - first_bias, width), F32))
        rows = jnp.concatenate(rows, axis=0).astype(BF16)
        sent = 0.5 * jnp.dot(rows, wsend_ref[...], preferred_element_type=F32)
        hi, lo = split(0.5 * bias_ref[...])
        row = lax.broadcasted_iota(jnp.int32, (WINDOW_ROWS, 1), 0)
        sent = jnp.where(row == first_bias, hi.astype(F32), sent)
        sent = jnp.where(row == first_bias + 1, lo.astype(F32), sent)
        rows_tab[height:, :] = jnp.concatenate(
            [sent, jnp.zeros((LANES - WINDOW_ROWS, width), F32)], axis=0
        ).astype(BF16)
        arrived(3, fetched)

    pieces = BLOCK // LANES
    each = SUB // LANES
    block = pl.ds(pl.multiple_of(step * BLOCK, BLOCK), BLOCK)
    near = table_rows(send_ref[:, block], mesh_rows, band, shards)
    near_lines = rows_of(near, pieces)
    recv_lines = rows_of(recv_ref[:, block], pieces)
    cols = columns_of(recv_lines + near_lines + rows_of(live_ref[:, block], pieces))
    lane = lax.broadcasted_iota(jnp.int32, (1, LANES), 1)
    always = jnp.where((lane == first_bias) | (lane == first_bias + 1), 1.0, 0.0)
    scale = 1.0 / width
    count = BLOCK // SUB
    spans = [range(part * each, (part + 1) * each) for part in range(count)]

    def hot_rows(span):
        hot = one_hot_rows([cols[i] for i in span], height)
        near = one_hot_rows([cols[pieces + i] for i in span], LANES, always)
        return hot, jnp.concatenate([hot, near], axis=1)

    def row_mean(x):
        return jnp.sum(x, axis=-1, keepdims=True) * scale

    ahead, behind = hot_rows(spans[0]), None
    for part in range(count + 1):
        if part < count:
            z = jnp.dot(ahead[1], rows_tab[...], preferred_element_type=F32)
            scaled = jnp.dot(ahead[0], cot_tab[...], preferred_element_type=F32)
        if behind is not None:
            span, hidden_b, slope_b, scaled_b, outer = behind
            live = jnp.concatenate([cols[2 * pieces + i] for i in span], axis=0)
            center = outer - row_mean(outer)
            inv = lax.rsqrt(row_mean(center * center) + 1e-05) * live
            normed = center * inv
            product = scaled_b * normed
            d_outer = scaled_b - row_mean(scaled_b) - normed * row_mean(product)
            d_outer = (d_outer * inv).astype(BF16)
            qacc[...] += groups(product)
            wsum[...] += mix(hidden_b, d_outer, 0, 0)
            d_hidden = mix(d_outer, wout_ref[...], 1, 1)
        if part < count:
            t = jnp.tanh(z)
            u = t + 1.0
            h = z * u
            hidden = h.astype(BF16)
            slope = u + h * (1.0 - t)
            outer = jnp.dot(hidden, wout_ref[...], preferred_element_type=F32)
        if behind is not None:
            d_pre = (d_hidden * slope_b).astype(BF16)
            hot = jnp.concatenate(
                [
                    one_hot_cols([recv_lines[i] for i in span], height),
                    one_hot_cols([near_lines[i] for i in span], WINDOW_ROWS),
                ],
                axis=0,
            )
            acc[...] += jnp.dot(hot, d_pre, preferred_element_type=F32)
        if part < count:
            behind = (spans[part], hidden, slope, scaled, outer)
        if part + 1 < count:
            ahead = hot_rows(spans[part + 1])

    @pl.when(step == pl.num_programs(0) - 1)
    def _():
        below = 0.5 * tacc[:mesh_rows, :]
        above = 0.5 * tacc[2 * mesh_rows : 3 * mesh_rows, :]
        own_ref[...] = 0.5 * tacc[mesh_rows : 2 * mesh_rows, :]
        up_ref[...] = jnp.where(even, above, below)
        edge = (band == 0) | (band == shards - 1)
        down_ref[...] = jnp.where(edge, 0.0, jnp.where(even, below, above))
        bias = 0.5 * jnp.sum(tacc[...], axis=0, keepdims=True)
        gain = jnp.sum(qacc[...], axis=0, keepdims=True) / gain_ref[...]
        gacc[...] = 0.5 * gacc[...]
        total[...] = mix(grid_ref[...], gacc[...].astype(BF16), 0, 0)
        half = (dkeep_ref.shape[0] - 8) // 2
        mine = pl.multiple_of(low * half, half) if halved else 0
        for k, whole in enumerate((wsum, total)):
            dkeep_ref[k * half : (k + 1) * half, :] = whole[pl.ds(mine, half), :]
            if halved:
                theirs = pl.multiple_of((1 - low) * half, half)
                dsend_ref[k * half : (k + 1) * half, :] = whole[pl.ds(theirs, half), :].astype(BF16)
        rest = jnp.zeros((4, width), F32)
        dkeep_ref[2 * half :, :] = jnp.concatenate([bias, gain, rest[:2], rest], axis=0)
        (bias_hi, bias_lo), (gain_hi, gain_lo) = split(bias), split(gain)
        sent = [v.astype(F32) for v in (bias_hi, gain_hi, bias_lo, gain_lo)]
        dsend_ref[dsend_ref.shape[0] - 8 :, :] = jnp.concatenate(sent + [rest], axis=0).astype(BF16)
        share = gkeep_ref.shape[1]
        for k in range(gkeep_ref.shape[0]):
            base = (high ^ k) * 2
            mine = pl.multiple_of((base + low) * share, share)
            theirs = pl.multiple_of((base + 1 - low) * share, share)
            gkeep_ref[k] = gacc[pl.ds(mine, share), :]
            gsend_ref[k] = gacc[pl.ds(theirs, share), :].astype(BF16)


def edges(shards, levels, place, pair, other, rows, cot, *fetched):
    send, grid = fetched[3], fetched[-1]
    slots = send.shape[1]
    height, width = grid.shape
    mesh_rows = pair.shape[0]
    halved = sliced(width, shards * levels)
    half = width // 2 if halved else width
    share = (levels // 2, height // levels, width)
    near = jax.ShapeDtypeStruct((mesh_rows, width), F32)
    outs = [
        jax.ShapeDtypeStruct(((width if halved else 0) + 8, width), BF16),
        jax.ShapeDtypeStruct((2 * half + 8, width), F32),
        jax.ShapeDtypeStruct(share, BF16),
        jax.ShapeDtypeStruct(share, F32),
        near, near, near,
    ]
    return pl.pallas_call(
        functools.partial(edge_kernel, shards, mesh_rows, halved, len(fetched)),
        grid=(slots // BLOCK,),
        in_specs=[pl.BlockSpec(memory_space=pltpu.SMEM), full(pair), full(other), full(rows), full(cot)]
        + [pl.BlockSpec(memory_space=pltpu.HBM)] * len(fetched),
        out_specs=[full(out) for out in outs],
        out_shape=outs,
        scratch_shapes=[pltpu.VMEM(array.shape, array.dtype) for array in fetched]
        + [
            pltpu.VMEM((height + LANES, width), BF16),
            pltpu.VMEM((width, width), F32),
            pltpu.VMEM((height + WINDOW_ROWS, width), F32),
            pltpu.VMEM((8, width), F32),
            pltpu.VMEM((width, width), F32),
            pltpu.SemaphoreType.DMA((len(fetched),)),
        ],
        compiler_params=pltpu.CompilerParams(vmem_limit_bytes=EDGE_VMEM),
        cost_estimate=cost(14 * slots * width * width, 16 * width * width),
        name="edges",
    )(place, pair, other, rows, cot, *held(fetched))


def combine_kernel(dkeep_ref, drecv_ref, gkeep_ref, grecv_ref, part_ref, gsend_ref, gown_ref):
    half = (dkeep_ref.shape[0] - 8) // 2
    width = dkeep_ref.shape[1]
    slab = half * width // LANES // part_ref.shape[0]
    for k in range(2):
        at = pl.ds(k * half, half)
        store_pieces(part_ref, k * slab, dkeep_ref[at, :] + drecv_ref[at, :].astype(F32))
    near = drecv_ref[2 * half :, :].astype(F32)
    vectors = dkeep_ref[2 * half : 2 * half + 2, :] + near[0:2] + near[2:4]
    extra = [tile for k in range(2) for tile in tiles_of(vectors[k : k + 1])]
    extra = jnp.concatenate(extra, axis=0).astype(BF16)
    part_ref[:, 2 * slab :, :] = jnp.broadcast_to(extra[None], (part_ref.shape[0],) + extra.shape)
    gown_ref[...] = gkeep_ref[0] + grecv_ref[0].astype(F32)
    gsend_ref[...] = (gkeep_ref[1] + grecv_ref[1].astype(F32)).astype(BF16)


def combine(parts, dkeep, drecv, gkeep, grecv):
    half, width = (dkeep.shape[0] - 8) // 2, dkeep.shape[1]
    rows = (2 * half // parts + 2) * (width // LANES)
    return pl.pallas_call(
        combine_kernel,
        out_shape=[
            jax.ShapeDtypeStruct((parts, rows, LANES), BF16),
            jax.ShapeDtypeStruct(gkeep.shape[1:], BF16),
            jax.ShapeDtypeStruct(gkeep.shape[1:], F32),
        ],
        compiler_params=pltpu.CompilerParams(vmem_limit_bytes=COMBINE_VMEM),
        cost_estimate=cost(2 * dkeep.size, 8 * dkeep.size),
        name="combine_halves",
    )(dkeep, drecv, gkeep, grecv)


def sum_kernel(
    part_ref, lat_ref, own_ref, pair_ref, other_ref, wsend_ref,
    pay_ref, dmesh_ref, dbias_ref, dgain_ref,
):
    tiles = dbias_ref.shape[1] // LANES
    slabs = part_ref.shape[1] - 2 * tiles
    total = jnp.sum(part_ref[...].astype(F32), axis=0)
    for k, ref in enumerate((dbias_ref, dgain_ref)):
        base = slabs + k * tiles
        both = total[base : base + tiles]
        for j in range(tiles):
            ref[:, j * LANES : (j + 1) * LANES] = both[j : j + 1]
    mesh = own_ref[...] + pair_ref[...] + other_ref[...]
    pieces = [total[:slabs]] + tiles_of(mesh) + tiles_of(lat_ref[...].astype(F32))
    payload = jnp.concatenate(pieces, axis=0).astype(BF16)
    pay_ref[...] = jnp.broadcast_to(payload[None], pay_ref.shape)
    dmesh_ref[...] = mix(mesh.astype(BF16), wsend_ref[...], 1, 1)


def sum_slabs(shards, part, lat, own, pair, other, wsend):
    mesh_rows, width = lat.shape
    tiles = width // LANES
    rows = part.shape[1] - 2 * tiles + 2 * mesh_rows * tiles
    vector = jax.ShapeDtypeStruct((1, width), F32)
    return pl.pallas_call(
        sum_kernel,
        out_shape=[
            jax.ShapeDtypeStruct((shards, rows, LANES), BF16),
            jax.ShapeDtypeStruct((mesh_rows, width), F32),
            vector, vector,
        ],
        compiler_params=pltpu.CompilerParams(vmem_limit_bytes=VMEM),
        cost_estimate=cost(2 * part.size, 4 * part.size),
        name="sum_slabs",
    )(part, lat, own, pair, other, wsend)


def spread_kernel(levels, mesh_rows, place_ref, *refs):
    parts_refs = refs[:levels]
    dsend_ref, drecv_ref, dout_ref, mesh, lat = refs[levels:]
    width = dsend_ref.shape[0]
    tiles = width // LANES
    shards = parts_refs[0].shape[0]
    own = width // (shards * levels)
    slab = own * tiles
    level = place_ref[1] * 2 + place_ref[2]
    for k, ref in enumerate(parts_refs):
        for s in range(shards):
            at = level ^ k
            high, low = lax.shift_right_logical(at, 1), at & 1
            place = (low * shards + s) * (levels // 2) + high
            tail = ref[s, 2 * slab :, :].astype(F32)
            rows = pl.ds(pl.multiple_of(place * own, own), own)
            near = pl.ds(pl.multiple_of(place * mesh_rows, mesh_rows), mesh_rows)
            for j in range(tiles):
                cols = pl.ds(j * LANES, LANES)
                dout_ref[rows, cols] = ref[s, j * own : (j + 1) * own, :]
                drecv_ref[rows, cols] = ref[s, slab + j * own : slab + (j + 1) * own, :]
                mesh[near, cols] = tail[j * mesh_rows : (j + 1) * mesh_rows]
                lat[near, cols] = tail[(tiles + j) * mesh_rows : (tiles + j + 1) * mesh_rows]
    dsend_ref[...] = mix(lat[...].astype(BF16), mesh[...].astype(BF16), 0, 0).astype(BF16)


def spread(width, mesh_rows, place, received):
    levels = len(received)
    rows = received[0].shape[0] * levels * mesh_rows
    out = jax.ShapeDtypeStruct((width, width), BF16)
    return pl.pallas_call(
        functools.partial(spread_kernel, levels, mesh_rows),
        in_specs=[pl.BlockSpec(memory_space=pltpu.SMEM)]
        + [pl.BlockSpec(memory_space=pltpu.VMEM)] * levels,
        out_shape=[out, out, out],
        scratch_shapes=[pltpu.VMEM((rows, width), F32)] * 2,
        compiler_params=pltpu.CompilerParams(vmem_limit_bytes=VMEM),
        cost_estimate=cost(2 * rows * width * width, 8 * width * width),
        name="spread_weights",
    )(place, *received)


def swap(x, axis, bit):
    return lax.ppermute(x, axis, [(i, i ^ bit) for i in range(lax.axis_size(axis))])


def swap_between(x, axis):
    count = lax.axis_size(axis)
    pairs = [(i, i + 1) for i in range(1, count - 1, 2)]
    ends = [(0, 0), (count - 1, count - 1)]
    return lax.ppermute(x, axis, pairs + [(j, i) for i, j in pairs] + ends)


def body(
    grid_latent, mesh_latent, grid_output_cotangent, w_send, w_recv, output_weight,
    hidden_layer_bias, output_norm_gain, edge_sender, edge_receiver, edge_live,
):
    shards, levels = lax.axis_size("space"), lax.axis_size("high") * 2
    parts = shards * levels
    width = grid_latent.shape[1]
    mesh_rows = mesh_latent.shape[1]
    lat = mesh_latent[0]
    whole_slabs = sliced(width, parts)
    place = jnp.stack([lax.axis_index(axis) for axis in ALL]).astype(jnp.int32)

    lat_pair = swap(lat, "space", 1)
    lat_other = swap_between(lat, "space")
    gain = output_norm_gain[None]
    rows, cot = tables(grid_latent, w_recv, grid_output_cotangent, gain)
    dsend, dkeep, gsend, gkeep, own, pair, other = edges(
        shards, levels, place, lat_pair, lat_other, rows, cot,
        w_send, lat, hidden_layer_bias[None], edge_sender, edge_receiver, edge_live,
        output_weight, gain, grid_latent,
    )
    pair = swap(pair, "space", 1)
    other = swap_between(other, "space")

    if not whole_slabs:
        rows = jnp.stack([gkeep.astype(BF16), gsend])
        for k in range(1, levels):
            side = rows[k % 2, k // 2]
            for bit in (1, 2):
                if k & bit:
                    side = swap(side, ("low", "high")[bit // 2], 1)
            gkeep = gkeep.at[0].add(side.astype(F32))
        d_grid = mix(gkeep[0].astype(BF16), w_recv, 1, 1)
        mesh = (own + pair + other).astype(BF16)
        d_mesh = mix(mesh, w_send, 1, 1)
        d_send, rest = lax.psum((mix(lat, mesh, 0, 0), dkeep), ALL)
        d_w_out, d_w_recv = rest[:width].astype(BF16), rest[width : 2 * width].astype(BF16)
        d_bias, d_gain = rest[2 * width], rest[2 * width + 1]
        return (d_grid, d_mesh[None], d_send.astype(BF16), d_w_recv, d_w_out, d_bias, d_gain)

    dnear = swap(dsend, "low", 1)
    gnear = swap(gsend, "low", 1)
    part, gsend, gown = combine(parts // 2, dkeep, dnear, gkeep, gnear)
    gfar = swap(gsend, "high", 1)
    part = lax.all_to_all(part, MOST, 0, 0, tiled=False)
    d_grid = mix((gown + gfar.astype(F32)).astype(BF16), w_recv, 1, 1)
    payload, d_mesh, d_bias, d_gain = sum_slabs(shards, part, lat, own, pair, other, w_send)
    received = {0: lax.all_to_all(payload, "space", 0, 0, tiled=False)}
    received[2] = swap(received[0], "high", 1)
    received[1] = swap(received[0], "low", 1)
    received[3] = swap(received[2], "low", 1)
    d_w_send, d_w_recv, d_w_out = spread(
        width, mesh_rows, place, [received[k] for k in range(levels)]
    )
    return (d_grid, d_mesh[None], d_w_send, d_w_recv, d_w_out, d_bias[0], d_gain[0])


def solution(mesh):
    shards, levels = mesh.devices.shape
    split_mesh = Mesh(mesh.devices.reshape(shards, levels // 2, 2), ALL)
    level = MOST[1:] + ALL[2:]

    return jax.shard_map(
        body,
        mesh=split_mesh,
        in_specs=(
            P("space", None), P(level, "space", None), P("space", None), P(), P(), P(), P(), P(),
            P(level, "space"), P(level, "space"), P(level, "space"),
        ),
        out_specs=(P(ALL, None), P(level, "space", None), P(), P(), P(), P(), P()),
        check_vma=False,
    )
```

```python
import functools

import jax
import jax.numpy as jnp
from jax import lax
from jax.experimental import pallas as pl
from jax.experimental.pallas import tpu as pltpu
from jax.sharding import Mesh, PartitionSpec as P


F32 = jnp.float32
BF16 = jnp.bfloat16
ALL = ("space", "high", "low")
MOST = ("space", "high")
LANES = 128
BLOCK = 2048
SUB = 256
WINDOW_ROWS = 32
VMEM = 16 * 1024 * 1024
EDGE_VMEM = 40 * 1024 * 1024
COMBINE_VMEM = 16 * 1024 * 1024


def sliced(width, parts):
    return width % (16 * parts) == 0


def cost(flops, nbytes):
    return pl.CostEstimate(flops=flops, bytes_accessed=nbytes, transcendentals=0)


def mix(a, b, left, right):
    return lax.dot_general(a, b, (((left,), (right,)), ((), ())), preferred_element_type=F32)


def full(array):
    return pl.BlockSpec(array.shape, lambda *_: (0,) * array.ndim)


def rows_of(line, count):
    return [line[:, j * LANES : (j + 1) * LANES] for j in range(count)]


def columns_of(lines):
    used = jnp.concatenate([line.astype(F32) for line in lines], axis=0)
    pad = jnp.zeros((LANES - used.shape[0], LANES), F32)
    turned = jnp.concatenate([used, pad], axis=0).T
    return [turned[:, j : j + 1] for j in range(len(lines))]


def one_hot_rows(columns, width, base=0.0):
    lane = lax.broadcasted_iota(jnp.int32, (LANES, width), 1).astype(F32)
    hot = [jnp.where(lane == column, 1.0, base).astype(BF16) for column in columns]
    return jnp.concatenate(hot, axis=0)


def one_hot_cols(lines, height):
    row = lax.broadcasted_iota(jnp.int32, (height, LANES), 0)
    hot = [jnp.where(row == line, 1.0, 0.0).astype(BF16) for line in lines]
    return jnp.concatenate(hot, axis=1)


def table_rows(sender, mesh_rows, band, shards):
    window = lax.div(sender, mesh_rows)
    target = band + window - 1
    window = jnp.where((target >= 0) & (target < shards), window, 1)
    return window * mesh_rows + lax.rem(sender, mesh_rows)


def groups(x):
    return jnp.sum(x.reshape(x.shape[0] // 8, 8, x.shape[1]), axis=0)


def split(x):
    hi = x.astype(BF16)
    return hi, (x - hi.astype(F32)).astype(BF16)


def store_pieces(out_ref, base, total):
    parts = out_ref.shape[0]
    own = total.shape[0] // parts
    for j, piece in enumerate(tiles_of(total)):
        at = pl.ds(base + j * own, own)
        out_ref[:, at, :] = piece.astype(BF16).reshape(parts, own, LANES)


def tiles_of(rows):
    return [rows[:, j : j + LANES] for j in range(0, rows.shape[1], LANES)]


def table_kernel(count, *refs):
    sources, (rows_ref, cot_tab_ref) = refs[:count], refs[count : count + 2]
    kept, copies, sems = refs[count + 2 : -5], refs[-5:-1], refs[-1]
    grid_ref, w_ref, cot_ref, gain_ref = copies
    targets = copies + kept
    moves = [pltpu.make_async_copy(sources[k], targets[k], sems.at[k]) for k in range(count)]
    for move in moves:
        move.start()
    for move in moves[:2]:
        move.wait()
    proj = jnp.dot(grid_ref[...], w_ref[...], preferred_element_type=F32)
    rows_ref[...] = (0.5 * proj).astype(BF16)
    for move in moves[2:4]:
        move.wait()
    cot_tab_ref[...] = (cot_ref[...].astype(F32) * gain_ref[...]).astype(BF16)
    for move in moves[4:]:
        move.wait()


def tables(grid, w, cot, gain, *kept):
    fetched = (grid, w, cot, gain) + kept
    out = jax.ShapeDtypeStruct(grid.shape, BF16)
    outs = [out, out] + [jax.ShapeDtypeStruct(array.shape, array.dtype) for array in kept]
    return pl.pallas_call(
        functools.partial(table_kernel, len(fetched)),
        in_specs=[pl.BlockSpec(memory_space=pltpu.HBM)] * len(fetched),
        out_specs=[pl.BlockSpec(memory_space=pltpu.VMEM)] * len(outs),
        out_shape=outs,
        scratch_shapes=[pltpu.VMEM(array.shape, array.dtype) for array in fetched[:4]]
        + [pltpu.SemaphoreType.DMA((len(fetched),))],
        compiler_params=pltpu.CompilerParams(vmem_limit_bytes=VMEM),
        cost_estimate=cost(2 * out.size * out.shape[1], 4 * out.size),
        name="tables",
    )(*held(fetched))


def held(arrays):
    return [pltpu.with_memory_space_constraint(array, pltpu.HBM) for array in arrays]


def edge_kernel(shards, mesh_rows, halved, fetched, place_ref, pair_ref, other_ref, rows_ref, cot_tab, *refs):
    (wsend_ref, wout_ref), refs = refs[:2], refs[2:]
    sources, refs = refs[:fetched], refs[fetched:]
    dsend_ref, dkeep_ref, gsend_ref, gkeep_ref, own_ref, up_ref, down_ref = refs[:7]
    copies, refs = refs[7 : 7 + fetched], refs[7 + fetched :]
    rows_tab, wsum, acc, qacc, total, sems = refs
    lat_ref, bias_ref, send_ref, recv_ref, live_ref, gain_ref, grid_ref = copies
    step = pl.program_id(0)
    band, high, low = place_ref[0], place_ref[1], place_ref[2]
    even = lax.rem(band, 2) == 0
    height, width = grid_ref.shape
    gacc, tacc = acc.at[:height, :], acc.at[height:, :]
    first_bias = 3 * mesh_rows

    def fetch(k):
        return pltpu.make_async_copy(sources[k], copies[k], sems.at[k])

    @pl.when(step == 0)
    def _():
        for k in range(fetched):
            fetch(k).start()

    def arrived(first, last):
        for k in range(first, last):
            fetch(k).wait()

    @pl.when(step == 0)
    def _():
        for ref in (wsum, acc, qacc):
            ref[...] = jnp.zeros_like(ref)
        rows_tab[:height, :] = rows_ref[...]
        arrived(0, 2)
        pair = pair_ref[...].astype(F32)
        other = other_ref[...].astype(F32)
        rows = [jnp.where(even, other, pair), lat_ref[...].astype(F32), jnp.where(even, pair, other)]
        rows.append(jnp.zeros((WINDOW_ROWS - first_bias, width), F32))
        rows = jnp.concatenate(rows, axis=0).astype(BF16)
        sent = 0.5 * jnp.dot(rows, wsend_ref[...], preferred_element_type=F32)
        hi, lo = split(0.5 * bias_ref[...])
        row = lax.broadcasted_iota(jnp.int32, (WINDOW_ROWS, 1), 0)
        sent = jnp.where(row == first_bias, hi.astype(F32), sent)
        sent = jnp.where(row == first_bias + 1, lo.astype(F32), sent)
        rows_tab[height:, :] = jnp.concatenate(
            [sent, jnp.zeros((LANES - WINDOW_ROWS, width), F32)], axis=0
        ).astype(BF16)
        arrived(2, fetched)

    pieces = BLOCK // LANES
    each = SUB // LANES
    block = pl.ds(pl.multiple_of(step * BLOCK, BLOCK), BLOCK)
    near = table_rows(send_ref[:, block], mesh_rows, band, shards)
    near_lines = rows_of(near, pieces)
    recv_lines = rows_of(recv_ref[:, block], pieces)
    cols = columns_of(recv_lines + near_lines + rows_of(live_ref[:, block], pieces))
    lane = lax.broadcasted_iota(jnp.int32, (1, LANES), 1)
    always = jnp.where((lane == first_bias) | (lane == first_bias + 1), 1.0, 0.0)
    scale = 1.0 / width
    count = BLOCK // SUB
    spans = [range(part * each, (part + 1) * each) for part in range(count)]

    def hot_rows(span):
        hot = one_hot_rows([cols[i] for i in span], height)
        near = one_hot_rows([cols[pieces + i] for i in span], LANES, always)
        return hot, jnp.concatenate([hot, near], axis=1)

    def row_mean(x):
        return jnp.sum(x, axis=-1, keepdims=True) * scale

    ahead, behind = hot_rows(spans[0]), None
    for part in range(count + 1):
        if part < count:
            z = jnp.dot(ahead[1], rows_tab[...], preferred_element_type=F32)
            scaled = jnp.dot(ahead[0], cot_tab[...], preferred_element_type=F32)
        if behind is not None:
            span, hidden_b, slope_b, scaled_b, outer = behind
            live = jnp.concatenate([cols[2 * pieces + i] for i in span], axis=0)
            center = outer - row_mean(outer)
            inv = lax.rsqrt(row_mean(center * center) + 1e-05) * live
            normed = center * inv
            product = scaled_b * normed
            d_outer = scaled_b - row_mean(scaled_b) - normed * row_mean(product)
            d_outer = (d_outer * inv).astype(BF16)
            qacc[...] += groups(product)
            wsum[...] += mix(hidden_b, d_outer, 0, 0)
            d_hidden = mix(d_outer, wout_ref[...], 1, 1)
        if part < count:
            t = jnp.tanh(z)
            u = t + 1.0
            h = z * u
            hidden = h.astype(BF16)
            slope = u + h * (1.0 - t)
            outer = jnp.dot(hidden, wout_ref[...], preferred_element_type=F32)
        if behind is not None:
            d_pre = (d_hidden * slope_b).astype(BF16)
            hot = jnp.concatenate(
                [
                    one_hot_cols([recv_lines[i] for i in span], height),
                    one_hot_cols([near_lines[i] for i in span], WINDOW_ROWS),
                ],
                axis=0,
            )
            acc[...] += jnp.dot(hot, d_pre, preferred_element_type=F32)
        if part < count:
            behind = (spans[part], hidden, slope, scaled, outer)
        if part + 1 < count:
            ahead = hot_rows(spans[part + 1])

    @pl.when(step == pl.num_programs(0) - 1)
    def _():
        below = 0.5 * tacc[:mesh_rows, :]
        above = 0.5 * tacc[2 * mesh_rows : 3 * mesh_rows, :]
        own_ref[...] = 0.5 * tacc[mesh_rows : 2 * mesh_rows, :]
        up_ref[...] = jnp.where(even, above, below)
        edge = (band == 0) | (band == shards - 1)
        down_ref[...] = jnp.where(edge, 0.0, jnp.where(even, below, above))
        bias = 0.5 * jnp.sum(tacc[...], axis=0, keepdims=True)
        gain = jnp.sum(qacc[...], axis=0, keepdims=True) / gain_ref[...]
        gacc[...] = 0.5 * gacc[...]
        total[...] = mix(grid_ref[...], gacc[...].astype(BF16), 0, 0)
        half = (dkeep_ref.shape[0] - 8) // 2
        mine = pl.multiple_of(low * half, half) if halved else 0
        for k, whole in enumerate((wsum, total)):
            dkeep_ref[k * half : (k + 1) * half, :] = whole[pl.ds(mine, half), :]
            if halved:
                theirs = pl.multiple_of((1 - low) * half, half)
                dsend_ref[k * half : (k + 1) * half, :] = whole[pl.ds(theirs, half), :].astype(BF16)
        rest = jnp.zeros((4, width), F32)
        dkeep_ref[2 * half :, :] = jnp.concatenate([bias, gain, rest[:2], rest], axis=0)
        (bias_hi, bias_lo), (gain_hi, gain_lo) = split(bias), split(gain)
        sent = [v.astype(F32) for v in (bias_hi, gain_hi, bias_lo, gain_lo)]
        dsend_ref[dsend_ref.shape[0] - 8 :, :] = jnp.concatenate(sent + [rest], axis=0).astype(BF16)
        share = gkeep_ref.shape[1]
        for k in range(gkeep_ref.shape[0]):
            base = (high ^ k) * 2
            mine = pl.multiple_of((base + low) * share, share)
            theirs = pl.multiple_of((base + 1 - low) * share, share)
            gkeep_ref[k] = gacc[pl.ds(mine, share), :]
            gsend_ref[k] = gacc[pl.ds(theirs, share), :].astype(BF16)


def edges(shards, levels, place, pair, other, rows, cot, wsend, wout, *fetched):
    send, grid = fetched[2], fetched[-1]
    ready = (pair, other, rows, cot, wsend, wout)
    slots = send.shape[1]
    height, width = grid.shape
    mesh_rows = pair.shape[0]
    halved = sliced(width, shards * levels)
    half = width // 2 if halved else width
    share = (levels // 2, height // levels, width)
    near = jax.ShapeDtypeStruct((mesh_rows, width), F32)
    outs = [
        jax.ShapeDtypeStruct(((width if halved else 0) + 8, width), BF16),
        jax.ShapeDtypeStruct((2 * half + 8, width), F32),
        jax.ShapeDtypeStruct(share, BF16),
        jax.ShapeDtypeStruct(share, F32),
        near, near, near,
    ]
    return pl.pallas_call(
        functools.partial(edge_kernel, shards, mesh_rows, halved, len(fetched)),
        grid=(slots // BLOCK,),
        in_specs=[pl.BlockSpec(memory_space=pltpu.SMEM), *map(full, ready)]
        + [pl.BlockSpec(memory_space=pltpu.HBM)] * len(fetched),
        out_specs=[full(out) for out in outs],
        out_shape=outs,
        scratch_shapes=[pltpu.VMEM(array.shape, array.dtype) for array in fetched]
        + [
            pltpu.VMEM((height + LANES, width), BF16),
            pltpu.VMEM((width, width), F32),
            pltpu.VMEM((height + WINDOW_ROWS, width), F32),
            pltpu.VMEM((8, width), F32),
            pltpu.VMEM((width, width), F32),
            pltpu.SemaphoreType.DMA((len(fetched),)),
        ],
        compiler_params=pltpu.CompilerParams(vmem_limit_bytes=EDGE_VMEM),
        cost_estimate=cost(14 * slots * width * width, 16 * width * width),
        name="edges",
    )(place, *ready, *held(fetched))


def combine_kernel(dkeep_ref, drecv_ref, gkeep_ref, grecv_ref, part_ref, gsend_ref, gown_ref):
    half = (dkeep_ref.shape[0] - 8) // 2
    width = dkeep_ref.shape[1]
    slab = half * width // LANES // part_ref.shape[0]
    for k in range(2):
        at = pl.ds(k * half, half)
        store_pieces(part_ref, k * slab, dkeep_ref[at, :] + drecv_ref[at, :].astype(F32))
    near = drecv_ref[2 * half :, :].astype(F32)
    vectors = dkeep_ref[2 * half : 2 * half + 2, :] + near[0:2] + near[2:4]
    extra = [tile for k in range(2) for tile in tiles_of(vectors[k : k + 1])]
    extra = jnp.concatenate(extra, axis=0).astype(BF16)
    part_ref[:, 2 * slab :, :] = jnp.broadcast_to(extra[None], (part_ref.shape[0],) + extra.shape)
    gown_ref[...] = gkeep_ref[0] + grecv_ref[0].astype(F32)
    gsend_ref[...] = (gkeep_ref[1] + grecv_ref[1].astype(F32)).astype(BF16)


def combine(parts, dkeep, drecv, gkeep, grecv):
    half, width = (dkeep.shape[0] - 8) // 2, dkeep.shape[1]
    rows = (2 * half // parts + 2) * (width // LANES)
    return pl.pallas_call(
        combine_kernel,
        out_shape=[
            jax.ShapeDtypeStruct((parts, rows, LANES), BF16),
            jax.ShapeDtypeStruct(gkeep.shape[1:], BF16),
            jax.ShapeDtypeStruct(gkeep.shape[1:], F32),
        ],
        compiler_params=pltpu.CompilerParams(vmem_limit_bytes=COMBINE_VMEM),
        cost_estimate=cost(2 * dkeep.size, 8 * dkeep.size),
        name="combine_halves",
    )(dkeep, drecv, gkeep, grecv)


def sum_kernel(
    part_ref, lat_ref, own_ref, pair_ref, other_ref, wsend_ref,
    pay_ref, dmesh_ref, dbias_ref, dgain_ref,
):
    tiles = dbias_ref.shape[1] // LANES
    slabs = part_ref.shape[1] - 2 * tiles
    total = jnp.sum(part_ref[...].astype(F32), axis=0)
    for k, ref in enumerate((dbias_ref, dgain_ref)):
        base = slabs + k * tiles
        both = total[base : base + tiles]
        for j in range(tiles):
            ref[:, j * LANES : (j + 1) * LANES] = both[j : j + 1]
    mesh = own_ref[...] + pair_ref[...] + other_ref[...]
    pieces = [total[:slabs]] + tiles_of(mesh) + tiles_of(lat_ref[...].astype(F32))
    payload = jnp.concatenate(pieces, axis=0).astype(BF16)
    pay_ref[...] = jnp.broadcast_to(payload[None], pay_ref.shape)
    dmesh_ref[...] = mix(mesh.astype(BF16), wsend_ref[...], 1, 1)


def sum_slabs(shards, part, lat, own, pair, other, wsend):
    mesh_rows, width = lat.shape
    tiles = width // LANES
    rows = part.shape[1] - 2 * tiles + 2 * mesh_rows * tiles
    vector = jax.ShapeDtypeStruct((1, width), F32)
    return pl.pallas_call(
        sum_kernel,
        out_shape=[
            jax.ShapeDtypeStruct((shards, rows, LANES), BF16),
            jax.ShapeDtypeStruct((mesh_rows, width), F32),
            vector, vector,
        ],
        compiler_params=pltpu.CompilerParams(vmem_limit_bytes=VMEM),
        cost_estimate=cost(2 * part.size, 4 * part.size),
        name="sum_slabs",
    )(part, lat, own, pair, other, wsend)


def spread_kernel(levels, mesh_rows, place_ref, *refs):
    parts_refs = refs[:levels]
    dsend_ref, drecv_ref, dout_ref, mesh, lat = refs[levels:]
    width = dsend_ref.shape[0]
    tiles = width // LANES
    shards = parts_refs[0].shape[0]
    own = width // (shards * levels)
    slab = own * tiles
    level = place_ref[1] * 2 + place_ref[2]
    for k, ref in enumerate(parts_refs):
        for s in range(shards):
            at = level ^ k
            high, low = lax.shift_right_logical(at, 1), at & 1
            place = (low * shards + s) * (levels // 2) + high
            tail = ref[s, 2 * slab :, :].astype(F32)
            rows = pl.ds(pl.multiple_of(place * own, own), own)
            near = pl.ds(pl.multiple_of(place * mesh_rows, mesh_rows), mesh_rows)
            for j in range(tiles):
                cols = pl.ds(j * LANES, LANES)
                dout_ref[rows, cols] = ref[s, j * own : (j + 1) * own, :]
                drecv_ref[rows, cols] = ref[s, slab + j * own : slab + (j + 1) * own, :]
                mesh[near, cols] = tail[j * mesh_rows : (j + 1) * mesh_rows]
                lat[near, cols] = tail[(tiles + j) * mesh_rows : (tiles + j + 1) * mesh_rows]
    dsend_ref[...] = mix(lat[...].astype(BF16), mesh[...].astype(BF16), 0, 0).astype(BF16)


def spread(width, mesh_rows, place, received):
    levels = len(received)
    rows = received[0].shape[0] * levels * mesh_rows
    out = jax.ShapeDtypeStruct((width, width), BF16)
    return pl.pallas_call(
        functools.partial(spread_kernel, levels, mesh_rows),
        in_specs=[pl.BlockSpec(memory_space=pltpu.SMEM)]
        + [pl.BlockSpec(memory_space=pltpu.VMEM)] * levels,
        out_shape=[out, out, out],
        scratch_shapes=[pltpu.VMEM((rows, width), F32)] * 2,
        compiler_params=pltpu.CompilerParams(vmem_limit_bytes=VMEM),
        cost_estimate=cost(2 * rows * width * width, 8 * width * width),
        name="spread_weights",
    )(place, *received)


def swap(x, axis, bit):
    return lax.ppermute(x, axis, [(i, i ^ bit) for i in range(lax.axis_size(axis))])


def swap_between(x, axis):
    count = lax.axis_size(axis)
    pairs = [(i, i + 1) for i in range(1, count - 1, 2)]
    ends = [(0, 0), (count - 1, count - 1)]
    return lax.ppermute(x, axis, pairs + [(j, i) for i, j in pairs] + ends)


def body(
    grid_latent, mesh_latent, grid_output_cotangent, w_send, w_recv, output_weight,
    hidden_layer_bias, output_norm_gain, edge_sender, edge_receiver, edge_live,
):
    shards, levels = lax.axis_size("space"), lax.axis_size("high") * 2
    parts = shards * levels
    width = grid_latent.shape[1]
    mesh_rows = mesh_latent.shape[1]
    lat = mesh_latent[0]
    whole_slabs = sliced(width, parts)
    place = jnp.stack([lax.axis_index(axis) for axis in ALL]).astype(jnp.int32)

    lat_pair = swap(lat, "space", 1)
    lat_other = swap_between(lat, "space")
    gain = output_norm_gain[None]
    ready = tables(
        grid_latent, w_recv, grid_output_cotangent, gain, w_send, output_weight
    )
    dsend, dkeep, gsend, gkeep, own, pair, other = edges(
        shards, levels, place, lat_pair, lat_other, *ready,
        lat, hidden_layer_bias[None], edge_sender, edge_receiver, edge_live,
        gain, grid_latent,
    )
    pair = swap(pair, "space", 1)
    other = swap_between(other, "space")

    if not whole_slabs:
        rows = jnp.stack([gkeep.astype(BF16), gsend])
        for k in range(1, levels):
            side = rows[k % 2, k // 2]
            for bit in (1, 2):
                if k & bit:
                    side = swap(side, ("low", "high")[bit // 2], 1)
            gkeep = gkeep.at[0].add(side.astype(F32))
        d_grid = mix(gkeep[0].astype(BF16), w_recv, 1, 1)
        mesh = (own + pair + other).astype(BF16)
        d_mesh = mix(mesh, w_send, 1, 1)
        d_send, rest = lax.psum((mix(lat, mesh, 0, 0), dkeep), ALL)
        d_w_out, d_w_recv = rest[:width].astype(BF16), rest[width : 2 * width].astype(BF16)
        d_bias, d_gain = rest[2 * width], rest[2 * width + 1]
        return (d_grid, d_mesh[None], d_send.astype(BF16), d_w_recv, d_w_out, d_bias, d_gain)

    dnear = swap(dsend, "low", 1)
    gnear = swap(gsend, "low", 1)
    part, gsend, gown = combine(parts // 2, dkeep, dnear, gkeep, gnear)
    gfar = swap(gsend, "high", 1)
    part = lax.all_to_all(part, MOST, 0, 0, tiled=False)
    d_grid = mix((gown + gfar.astype(F32)).astype(BF16), w_recv, 1, 1)
    payload, d_mesh, d_bias, d_gain = sum_slabs(shards, part, lat, own, pair, other, w_send)
    received = {0: lax.all_to_all(payload, "space", 0, 0, tiled=False)}
    received[2] = swap(received[0], "high", 1)
    received[1] = swap(received[0], "low", 1)
    received[3] = swap(received[2], "low", 1)
    d_w_send, d_w_recv, d_w_out = spread(
        width, mesh_rows, place, [received[k] for k in range(levels)]
    )
    return (d_grid, d_mesh[None], d_w_send, d_w_recv, d_w_out, d_bias[0], d_gain[0])


def solution(mesh):
    shards, levels = mesh.devices.shape
    split_mesh = Mesh(mesh.devices.reshape(shards, levels // 2, 2), ALL)
    level = MOST[1:] + ALL[2:]

    return jax.shard_map(
        body,
        mesh=split_mesh,
        in_specs=(
            P("space", None), P(level, "space", None), P("space", None), P(), P(), P(), P(), P(),
            P(level, "space"), P(level, "space"), P(level, "space"),
        ),
        out_specs=(P(ALL, None), P(level, "space", None), P(), P(), P(), P(), P()),
        check_vma=False,
    )
```
